256 devices in a mesh: facet: 64 (over z, x, core), stokes: 4 (over y).
Axes of the slice: x: 4, y: 4, z: 8, core: 2. Of those that a mesh axis runs over, the one named last changes fastest.
Arguments:
- strips: bfloat16 [4, 4096, 16384], P('stokes', 'facet'), may hold values from -6 to 6
- sub_u: int32 [128], replicated, may hold values from 0 to 4095
- counts: int32 [128], P('facet'), may hold values from 1 to 64, 4096 in all
- uvw: int32 [3, 128, 8192], P(None, 'facet'), may hold values from 0 to 255
- mueller: float32 [4, 4, 128, 64], P(None, None, 'facet'), may hold values from -3 to 3
- observed: float32 [4, 128, 2, 8192], P('stokes', 'facet'), may hold values from -6 to 6
Outputs:
- image_out: bfloat16 [4, 4096, 16384], P('stokes', 'facet')
- residual_vis: float32 [4, 128, 2, 8192], P('stokes', 'facet')
The draws below stay inside these ranges and needn't reach their ends.
Inputs may be any that keep to these rules, and one draw needn't show every extreme that they name: Block counts of one subgrid are at most 64; some subgrid has exactly 64.
All inputs are finite; a program needn't handle non-finite values.
Results may differ from the reference program's by a relative error of at most 0.018.
Values may be sent and summed in bfloat16 or wider, within the bound.
No kernel may reach another device: no remote copies, remote signals or barrier semaphores. Data moves between devices by JAX's collectives and lax.ppermute only.
A program may use at most 128 MiB of HBM per device.

```python
import math
import jax
import jax.numpy as jnp
import numpy as np
from jax import lax

RF = 64
L = 8192
K = 64
G = 256
MAXB = 64
BLOCK = 128
VISITS = 8192
NSUB = 128
NR = 4096
N_FACET = 64


def set_ends(values, key, least, high):
    place = [jax.random.randint(jax.random.fold_in(key, axis), (), 0, length) for axis, length in enumerate(values.shape)]
    main_axis = values.shape.index(max(values.shape))
    beside = place[:main_axis] + [(place[main_axis] + 1) % values.shape[main_axis]] + place[main_axis + 1:]
    return values.at[tuple(place)].set(least).at[tuple(beside)].set(high)


def steps_of(rng, shape, cuts, smallest, high):
    loudness, own = 1.0, jax.random.fold_in(rng, 6)
    for dim, parts in cuts:
        draws = jnp.exp(jax.random.uniform(jax.random.fold_in(own, dim), (parts,), jnp.float32, smallest / len(cuts), high / len(cuts)))
        loudness = loudness * jnp.repeat(draws, shape[dim] // parts).reshape([-1 if axis == dim else 1 for axis in range(len(shape))])
    return loudness


def profile(amount, total, reach, lean):
    weights = [(1 << 20) // math.isqrt(rank ** lean) + 1 for rank in range(2, amount + 1)]
    surplus, given = total - reach - (amount - 1), [1] * (amount - 1)
    while surplus > 0:
        free = [i for i in range(amount - 1) if given[i] < reach]
        mass, remaining = sum([weights[i] for i in free]), surplus
        for i in free:
            addition = min(reach - given[i], max(1, remaining * weights[i] // mass), surplus)
            given[i] = given[i] + addition
            surplus = surplus - addition
    return np.array([reach] + given)


def ragged(own_key, number_of, total, reach, lean):
    if number_of == 2:
        one = jax.random.randint(own_key, (), max(1, total - reach), min(reach, total - 1) + 1)
        return jnp.stack([one, total - one])
    lengths = jnp.asarray(profile(number_of, total, reach, lean), jnp.int32)
    twos = (number_of - 1) // 2
    source_of, receiver = lengths[1:1 + 2 * twos:2], lengths[2:2 + 2 * twos:2]
    margin = jnp.minimum(source_of - 1, reach - receiver)
    shifted = jax.random.randint(jax.random.fold_in(own_key, 1), (twos,), 0, 1 << 20) % (margin + 1)
    lengths = lengths.at[1:1 + 2 * twos:2].set(source_of - shifted).at[2:2 + 2 * twos:2].set(receiver + shifted)
    return lengths[jax.random.permutation(jax.random.fold_in(own_key, 2), number_of)]


def normal_values(rng, extent, deviation, bound, split=(), kind=jnp.bfloat16):
    loudness = steps_of(rng, extent, split, -0.22, 0.18) if split else 1.0
    entries = jax.random.normal(rng, extent, jnp.float32) * deviation * loudness
    return jnp.minimum(jnp.maximum(entries, -bound), bound).astype(kind)


def setup_inputs(seed: int = 0) -> dict:
    seeds = jax.random.split(jax.random.key(seed), 7)
    strips = normal_values(seeds[0], (4, NR, 2 * L), 1.0, 6.0, ((0, 4), (1, 64)))
    sub_u = set_ends(jax.random.randint(seeds[1], (NSUB,), 0, NR), jax.random.fold_in(seeds[1], 1), 0, NR - 1).astype(jnp.int32)
    counts = ragged(seeds[2], NSUB, NSUB * MAXB // 2, MAXB, 2).astype(jnp.int32)
    uvw = set_ends(jax.random.randint(seeds[3], (3, NSUB, VISITS), 0, G), jax.random.fold_in(seeds[3], 1), 0, G - 1).astype(jnp.int32)
    mueller = normal_values(seeds[4], (4, 4, NSUB, MAXB), 0.6, 3.0, ((2, 64),), jnp.float32)
    observed = normal_values(seeds[5], (4, NSUB, 2, VISITS), 1.0, 6.0, ((0, 4), (1, 64)), jnp.float32)
    return {"strips": strips, "sub_u": sub_u, "counts": counts, "uvw": uvw, "mueller": mueller, "observed": observed}


full_turn = 2.0 * math.pi

def turn(phase, period):
    angle = phase.astype(jnp.float32) * (full_turn / period)
    return (jnp.cos(angle), jnp.sin(angle))

def lower(value):
    return lax.optimization_barrier(value.astype(jnp.bfloat16))

def stack_right(real, imag):
    return jnp.concatenate([jnp.concatenate([real, imag], 1), jnp.concatenate([-imag, real], 1)], 0)

def column_table(length, samples):
    lpos = jnp.arange(length, dtype=jnp.int32)[:, None]
    cpos = jnp.arange(samples, dtype=jnp.int32)[None, :]
    cosine, sine = turn(4 * cpos * lpos % length, length)
    scale = 1.0 / math.sqrt(length)
    return stack_right(cosine * scale, -sine * scale).astype(jnp.bfloat16)

def interp_table(width, samples):
    upos = jnp.arange(width, dtype=jnp.int32)[:, None, None]
    kpos = jnp.arange(samples, dtype=jnp.int32)[None, :, None]
    mpos = jnp.arange(samples, dtype=jnp.int32)[None, None, :] - samples // 2
    cosine, sine = turn(jnp.remainder(mpos * (upos - 4 * kpos), width), width)
    return (lax.optimization_barrier(jnp.sum(cosine, 2)) / (2.0 * samples), lax.optimization_barrier(jnp.sum(sine, 2)) / (2.0 * samples))

def facet_table(real, imag, facets, rows, total):
    width, samples = real.shape
    centre = (facets * rows + rows // 2)[None, :, None]
    upos = jnp.arange(width, dtype=jnp.int32)[:, None, None]
    kpos = jnp.arange(samples, dtype=jnp.int32)[None, None, :]
    phase = 4 * kpos * centre % total - upos * centre % total
    cosine, sine = turn(phase, total)
    e_real = real[:, None, :] * cosine - imag[:, None, :] * sine
    e_imag = real[:, None, :] * sine + imag[:, None, :] * cosine
    return (e_real, e_imag)

def row_table(offsets, positions, total, samples):
    kpos = jnp.arange(samples, dtype=jnp.int32)
    freq = (offsets[:, None] + 4 * kpos[None, :]) % total
    phase = freq[:, :, None] * positions[None, None, :] % total
    cosine, sine = turn(phase, total)
    scale = 1.0 / math.sqrt(total)
    return (cosine * scale, -sine * scale)

def join(first, second, conj):
    half = first.shape[-1] // 2
    if conj:
        real = first[..., :half] + second[..., half:]
        imag = first[..., half:] - second[..., :half]
    else:
        real = first[..., :half] - second[..., half:]
        imag = first[..., half:] + second[..., :half]
    return jnp.concatenate([real, imag], -1)

def cein(form, left_re, left_im, packed, conj):
    hp = lax.Precision.HIGHEST
    right = packed.astype(jnp.float32)
    first = jnp.einsum(form, left_re.astype(jnp.float32), right, precision=hp)
    second = jnp.einsum(form, left_im.astype(jnp.float32), right, precision=hp)
    return join(first, second, conj)

def reference(strips, sub_u, counts, uvw, mueller, observed):
    total = RF * N_FACET
    hp = lax.Precision.HIGHEST
    column = column_table(L, K)
    coeffs = lower(jnp.dot(strips, column, preferred_element_type=jnp.float32))
    blocked = coeffs.reshape(4, N_FACET, RF, 2 * K)
    b_re, b_im = interp_table(G, K)
    e_re, e_im = facet_table(b_re, b_im, jnp.arange(N_FACET, dtype=jnp.int32), RF, total)
    e_re = lower(e_re)
    e_im = lower(e_im)
    lb_re = lower(b_re).astype(jnp.float32)
    lb_im = lower(b_im).astype(jnp.float32)
    s_tab = stack_right(lb_re.T, lb_im.T)
    positions = jnp.arange(total, dtype=jnp.int32)
    blocks = jnp.arange(MAXB, dtype=jnp.int32)

    def one_subgrid(carry, items):
        offset, count, coords, mix, seen = items
        r_re, r_im = row_table(offset[None], positions, total, K)
        r_re = lower(r_re.reshape(K, N_FACET, RF))
        r_im = lower(r_im.reshape(K, N_FACET, RF))
        patches = lower(cein('kfr,sfrc->sfkc', r_re, r_im, blocked, False))
        lifted = lower(cein('ufk,sfkc->suc', e_re, e_im, patches, False))
        subgrid = jnp.einsum('sux,xy->suy', lifted.astype(jnp.float32), s_tab, precision=hp)
        flat = subgrid.reshape(4, G * 2 * G)
        index = (coords[0] * (2 * G) + coords[1]).astype(jnp.int32)
        m_re = flat[:, index]
        m_im = flat[:, index + G]
        cosine, sine = turn(coords[2], G)
        mod_re = m_re * cosine + m_im * sine
        mod_im = m_im * cosine - m_re * sine
        model = jnp.stack([mod_re, mod_im], 1).reshape(4, 2, MAXB, BLOCK)
        corr = lax.optimization_barrier(jnp.sum(mix[:, :, None, :, None] * model[None], axis=1))
        live = (blocks < count).astype(jnp.float32)[None, None, :, None]
        resid = (seen.reshape(4, 2, MAXB, BLOCK) - corr) * live
        back = lax.optimization_barrier(jnp.sum(mix[:, :, None, :, None] * resid[:, None], axis=0)).reshape(4, 2, VISITS)
        g_re = back[:, 0] * cosine - back[:, 1] * sine
        g_im = back[:, 1] * cosine + back[:, 0] * sine
        w_re = lb_re[coords[1]][None]
        w_im = lb_im[coords[1]][None]
        v_re = g_re[..., None] * w_re + g_im[..., None] * w_im
        v_im = g_im[..., None] * w_re - g_re[..., None] * w_im
        terms = lower(jnp.concatenate([v_re, v_im], -1)).astype(jnp.float32)
        lifted_adj = lower(jnp.zeros((4, G, 2 * K), jnp.float32).at[:, coords[0]].add(terms))
        patches_adj = lower(cein('ufk,suc->sfkc', e_re, e_im, lifted_adj, True))
        contrib = cein('kfr,sfkc->sfrc', r_re, r_im, patches_adj, True)
        return (carry + contrib.reshape(4, total, 2 * K), resid.reshape(4, 2, VISITS))
    items = (sub_u, counts, jnp.transpose(uvw, (1, 0, 2)), jnp.transpose(mueller, (2, 0, 1, 3)), jnp.transpose(observed, (1, 0, 2, 3)))
    sums, resids = lax.scan(one_subgrid, jnp.zeros((4, total, 2 * K), jnp.float32), items)
    image = lax.dot_general(sums.astype(jnp.bfloat16), column, (((2,), (1,)), ((), ())), preferred_element_type=jnp.float32)
    image_out = (8.0 * image).astype(jnp.bfloat16)
    return (image_out, jnp.transpose(resids, (1, 0, 2, 3)))
```

```python
import functools
import math

import jax
import jax.numpy as jnp
import numpy as np
from jax import lax
from jax.experimental import pallas as pl
from jax.experimental.pallas import tpu as pltpu
from jax.sharding import PartitionSpec as P

K = 64
G = 256
L = 8192
PERIOD = 2048
ROWS = 64
FACETS = 64
TOTAL = 4096
MAXB = 64
BLOCK = 128
VISITS = 8192
CHUNK = 512

f32 = jnp.float32
bf16 = jnp.bfloat16


@functools.cache
def tables():
    lpos = np.arange(PERIOD)[None, :]
    cpos = np.arange(K)[:, None]
    angle = 2.0 * np.pi * ((4 * cpos * lpos) % L) / L
    column = np.concatenate([np.cos(angle), -np.sin(angle)], 0) / math.sqrt(L)
    upos = np.arange(G)[:, None]
    kpos = np.arange(K)[None, :]
    mpos = np.arange(K) - K // 2
    phase = (mpos[None, None, :] * (upos - 4 * kpos)[:, :, None]) % G
    interp = np.exp(2j * np.pi * phase / G).sum(2) / (2.0 * K)
    interp_t = np.concatenate([interp.real.T, interp.imag.T], 0)
    dpos = np.arange(ROWS) - ROWS // 2
    lift = interp @ np.exp(-2j * np.pi * np.arange(K)[:, None] * dpos[None, :] / 1024)
    lift = lift * np.exp(-2j * np.pi * upos / 128) / math.sqrt(TOTAL)
    lift_t = np.concatenate([lift.real.T, lift.imag.T], 0)
    lift_s = np.concatenate([-lift.imag.T, lift.real.T], 0)
    return (
        column.astype(np.float32),
        interp_t.astype(np.float32),
        lift_t.astype(np.float32),
        lift_s.astype(np.float32),
    )


def half_sign():
    lane = lax.broadcasted_iota(jnp.int32, (1, 2 * K), 1)
    return jnp.where(lane < K, 1.0, -1.0).astype(f32)


def swap(x):
    return pltpu.roll(x, K, 1)


def one_hot(cells):
    grid_pos = lax.broadcasted_iota(jnp.int32, (G, cells.shape[1]), 0)
    return jnp.where(grid_pos == cells, 1.0, 0.0).astype(bf16)


def nt_dot(a, b):
    return lax.dot_general(a, b, (((1,), (1,)), ((), ())), preferred_element_type=f32)


def column_kernel(strips_ref, column_ref, out_ref):
    parts = []
    for base in (0, L):
        folded = strips_ref[:, base : base + PERIOD].astype(f32)
        for turn in range(1, 4):
            start = base + turn * PERIOD
            folded = folded + strips_ref[:, start : start + PERIOD].astype(f32)
        parts.append(folded.astype(bf16))
    product = nt_dot(column_ref[...], jnp.concatenate(parts, 0))
    out_ref[...] = (product[:K] - half_sign() * swap(product[K:])).astype(bf16)


def weights_kernel(cells_ref, interp_ref, out_ref):
    for sub in range(2):

        def chunk(n, carry):
            at = pl.ds(pl.multiple_of(n * CHUNK, CHUNK), CHUNK)
            picked = jnp.dot(
                interp_ref[...], one_hot(cells_ref[1, sub : sub + 1, at]), preferred_element_type=f32
            )
            out_ref[sub, :, at] = picked.astype(bf16)
            return carry

        lax.fori_loop(0, VISITS // CHUNK, chunk, 0, unroll=2)


def facet_lift(cos_row, sin_row, lift_ref, lift_s_ref):
    return (cos_row * lift_ref[...] + sin_row * lift_s_ref[...]).astype(bf16)


def model_kernel(
    mine_ref, other_ref, cos_ref, sin_ref, fcos_ref, fsin_ref, lift_ref, lift_s_ref, cells_ref,
    weights_ref, seen_ref, out_ref, rows_ref, lifted_ref, samples_ref,
):
    sign = half_sign()
    rows_ref[...] = jnp.zeros_like(rows_ref)
    for side, source in enumerate((mine_ref, other_ref)):

        def pair(i, carry):
            lefts, rights = [], []
            for e in range(2):
                q = 2 * i + e
                p = side * 32 + q
                first = source[q].astype(f32)
                second = swap(first)
                rights.append(
                    facet_lift(fcos_ref[pl.ds(p, 1), :], fsin_ref[pl.ds(p, 1), :], lift_ref, lift_s_ref)
                )
                blocks = []
                for sub in range(2):
                    pr = cos_ref[pl.ds(sub * FACETS + p, 1), :]
                    pi = sin_ref[pl.ds(sub * FACETS + p, 1), :]
                    blocks.append((first * (pr * sign) - second * pi).astype(bf16))
                    blocks.append((second * pr + first * (pi * sign)).astype(bf16))
                lefts.append(jnp.concatenate(blocks, 0))
            left = jnp.concatenate(lefts, 1)
            right = jnp.concatenate(rights, 0)
            rows_ref[...] += jnp.dot(left, right, preferred_element_type=f32)
            return carry

        lax.fori_loop(0, 16, pair, 0, unroll=2)
    lifted_ref[...] = rows_ref[...].astype(bf16)
    per = CHUNK // BLOCK
    for sub in range(2):

        def chunk(n, carry):
            at = pl.ds(pl.multiple_of(n * CHUNK, CHUNK), CHUNK)
            picked = jnp.dot(
                lifted_ref[sub * 2 * K : (sub + 1) * 2 * K, :],
                one_hot(cells_ref[0, sub : sub + 1, at]),
                preferred_element_type=f32,
            )
            w_re = weights_ref[sub, :K, at].astype(f32)
            w_im = weights_ref[sub, K:, at].astype(f32)
            y_re, y_im = picked[:K], picked[K:]
            m_re = jnp.sum(y_re * w_re - y_im * w_im, 0, keepdims=True)
            m_im = jnp.sum(y_re * w_im + y_im * w_re, 0, keepdims=True)
            for b in range(per):
                lanes = slice(b * BLOCK, (b + 1) * BLOCK)
                samples_ref[pl.ds(2 * sub * MAXB + n * per + b, 1), :] = m_re[:, lanes]
                samples_ref[pl.ds((2 * sub + 1) * MAXB + n * per + b, 1), :] = m_im[:, lanes]
            return carry

        lax.fori_loop(0, VISITS // CHUNK, chunk, 0, unroll=2)
    out_ref[: 4 * MAXB, :] = samples_ref[...].astype(bf16)
    out_ref[4 * MAXB :, :] = seen_ref[...].astype(bf16)


def residual_kernel(
    counts_ref, a_ref, b_ref, c_ref, d_ref, seen_ref, mix_ref, cos_ref, sin_ref, cells_ref, weights_ref,
    resid_ref, out_ref, back_ref,
):
    planes = (a_ref, b_ref, c_ref, d_ref)
    block = lax.broadcasted_iota(jnp.int32, (MAXB, BLOCK), 0)
    for sub in range(2):
        live = block < counts_ref[sub]
        here = slice(sub * MAXB, (sub + 1) * MAXB)
        re = slice(2 * sub * MAXB, (2 * sub + 1) * MAXB)
        im = slice((2 * sub + 1) * MAXB, (2 * sub + 2) * MAXB)
        seen_re = slice(4 * MAXB + re.start, 4 * MAXB + re.stop)
        seen_im = slice(4 * MAXB + im.start, 4 * MAXB + im.stop)
        cosine, sine = cos_ref[here, :], sin_ref[here, :]
        s_re = [p[re, :].astype(f32) for p in planes]
        s_im = [p[im, :].astype(f32) for p in planes]
        back_re = jnp.zeros((MAXB, BLOCK), f32)
        back_im = jnp.zeros((MAXB, BLOCK), f32)
        for corr in range(4):
            mix = [mix_ref[here, 4 * corr + t : 4 * corr + t + 1] for t in range(4)]
            m_re = sum(m * s for m, s in zip(mix, s_re))
            m_im = sum(m * s for m, s in zip(mix, s_im))
            o_re = seen_ref[re, :] if corr == 0 else planes[corr][seen_re, :].astype(f32)
            o_im = seen_ref[im, :] if corr == 0 else planes[corr][seen_im, :].astype(f32)
            r_re = jnp.where(live, o_re - (m_re * cosine + m_im * sine), 0.0)
            r_im = jnp.where(live, o_im - (m_im * cosine - m_re * sine), 0.0)
            if corr == 0:
                resid_ref[re, :] = r_re
                resid_ref[im, :] = r_im
            back_re = back_re + mix[0] * r_re
            back_im = back_im + mix[0] * r_im
        back_ref[re, :] = back_re * cosine - back_im * sine
        back_ref[im, :] = back_im * cosine + back_re * sine
    per = CHUNK // BLOCK
    for sub in range(2):

        def chunk(n, total):
            at = pl.ds(pl.multiple_of(n * CHUNK, CHUNK), CHUNK)

            def row(part):
                base = (2 * sub + part) * MAXB + n * per
                return jnp.concatenate([back_ref[pl.ds(base + b, 1), :] for b in range(per)], 1)

            g_re, g_im = row(0), row(1)
            w_re = weights_ref[sub, :K, at].astype(f32)
            w_im = weights_ref[sub, K:, at].astype(f32)
            v_re = (g_re * w_re + g_im * w_im).astype(bf16)
            v_im = (g_im * w_re - g_re * w_im).astype(bf16)
            return total + nt_dot(one_hot(cells_ref[0, sub : sub + 1, at]), jnp.concatenate([v_re, v_im], 0))

        total = lax.fori_loop(0, VISITS // CHUNK, chunk, jnp.zeros((G, 2 * K), f32), unroll=2)
        out_ref[sub * 2 * K : (sub + 1) * 2 * K, :] = jnp.transpose(total).astype(bf16)


def share_kernel(
    mine_ref, other_ref, cos_ref, sin_ref, fcos_ref, fsin_ref, lift_ref, lift_s_ref, out_ref
):
    sign = half_sign()
    left = jnp.concatenate([mine_ref[...], other_ref[...]], 0)

    def pair(i, carry):
        rights = []
        for e in range(2):
            q = 2 * i + e
            rights.append(
                facet_lift(fcos_ref[pl.ds(q, 1), :], fsin_ref[pl.ds(q, 1), :], lift_ref, lift_s_ref)
            )
        product = nt_dot(left, jnp.concatenate(rights, 0))
        for e in range(2):
            q = 2 * i + e
            total = jnp.zeros((K, 2 * ROWS), f32)
            for sub in range(4):
                g_re = product[sub * 2 * K : sub * 2 * K + K, e * 128 : (e + 1) * 128]
                g_im = product[sub * 2 * K + K : (sub + 1) * 2 * K, e * 128 : (e + 1) * 128]
                g_re = g_re * sign
                pr = cos_ref[pl.ds(sub * 32 + q, 1), :]
                pi = sin_ref[pl.ds(sub * 32 + q, 1), :]
                total = total + (g_re + swap(g_im)) * pr + (swap(g_re) + g_im) * (pi * sign)
            out_ref[q] = total.astype(bf16)
        return carry

    lax.fori_loop(0, 16, pair, 0, unroll=2)


def image_kernel(shares_ref, column_ref, out_ref):
    total = shares_ref[0].astype(f32)
    for q in range(1, 32):
        total = total + shares_ref[q].astype(f32)
    total = total.astype(bf16).astype(f32)
    both = jnp.concatenate([total, half_sign() * swap(total)], 0)
    left = jnp.transpose(both).astype(bf16)
    image = (8.0 * jnp.dot(left, column_ref[...], preferred_element_type=f32)).astype(bf16)
    for turn in range(4):
        out_ref[:, turn * PERIOD : (turn + 1) * PERIOD] = image[:ROWS]
        out_ref[:, L + turn * PERIOD : L + (turn + 1) * PERIOD] = image[ROWS:]


def call(kernel, out_shape, scratch=(), smem=0, count=1):
    vmem = pl.BlockSpec(memory_space=pltpu.VMEM)

    def run(*args):
        specs = [pl.BlockSpec(memory_space=pltpu.SMEM)] * smem + [vmem] * (len(args) - smem)
        return pl.pallas_call(
            kernel,
            out_shape=out_shape,
            in_specs=specs,
            out_specs=jax.tree.map(lambda _: vmem, out_shape),
            scratch_shapes=list(scratch),
        )(*args)

    return run


def shape(dims, dtype):
    return jax.ShapeDtypeStruct(dims, dtype)


def turn(phase, period):
    angle = phase.astype(f32) * (2.0 * math.pi / period)
    return (jnp.cos(angle), -jnp.sin(angle))


def row_phases(offsets, facets):
    rows = facets[:, None] * ROWS + jnp.tile(jnp.arange(ROWS, dtype=jnp.int32), 2)[None, :]
    phase = (offsets[:, None, None] * rows[None]) % TOTAL
    cosine, sine = turn(phase.reshape(-1, 2 * ROWS), TOTAL)
    return (cosine, sine)


def facet_phases(facets):
    phase = (facets[:, None] * jnp.arange(G, dtype=jnp.int32)[None, :]) % FACETS
    return turn(phase, FACETS)


def body(strips, sub_u, counts, uvw, mueller, observed):
    column, interp_t, lift_t, lift_s = tables()
    column = jnp.asarray(column, bf16)
    interp_t = jnp.asarray(interp_t, bf16)
    lift_t = jnp.asarray(lift_t)
    lift_s = jnp.asarray(lift_s)
    here = lax.axis_index("facet")
    plane = lax.axis_index("stokes")
    core = here % 2
    groups = [[2 * q + side for q in range(32)] for side in range(2)]
    partner = [(i, i ^ 1) for i in range(FACETS)]
    step = jnp.arange(32, dtype=jnp.int32)

    coeffs = call(column_kernel, shape((K, 2 * ROWS), bf16))(strips[0], column)
    spread = jnp.broadcast_to(coeffs[None], (32, K, 2 * ROWS))
    mine = lax.all_to_all(spread, "facet", 0, 0, axis_index_groups=groups, tiled=True)
    other = lax.ppermute(mine, "facet", partner)

    weights = call(weights_kernel, shape((2, 2 * K, VISITS), bf16))(uvw, interp_t)
    own_facets = 2 * step + core
    other_facets = 2 * step + 1 - core
    offsets = lax.dynamic_slice_in_dim(sub_u, 2 * here, 2)
    other_offsets = lax.dynamic_slice_in_dim(sub_u, 2 * (here + 1 - 2 * core), 2)
    all_facets = jnp.concatenate([own_facets, other_facets])
    cos_f, sin_f = row_phases(offsets, all_facets)
    cos_a, sin_a = row_phases(jnp.concatenate([offsets, other_offsets]), own_facets)
    fcos, fsin = facet_phases(all_facets)
    seen = observed.reshape(4 * MAXB, BLOCK)
    vcos, vsin = turn(uvw[2].reshape(2 * MAXB, BLOCK), G)
    vsin = -vsin
    mix = jnp.concatenate([mueller, mueller], 0)
    mix = jnp.concatenate([mix, mix], 1)
    mix = lax.dynamic_slice(mix, (plane, plane, 0, 0), (4, 4, 2, MAXB))
    mix = jnp.transpose(mix.reshape(16, 2 * MAXB))

    sent = call(
        model_kernel,
        shape((8 * MAXB, BLOCK), bf16),
        (
            pltpu.VMEM((4 * K, G), f32),
            pltpu.VMEM((4 * K, G), bf16),
            pltpu.VMEM((4 * MAXB, BLOCK), f32),
        ),
    )(mine, other, cos_f, sin_f, fcos, fsin, lift_t, lift_s, uvw, weights, seen)
    planes = [sent] + [
        lax.ppermute(sent, "stokes", [(i, (i - k) % 4) for i in range(4)]) for k in (1, 2, 3)
    ]
    resid, adj = call(
        residual_kernel,
        (shape((4 * MAXB, BLOCK), f32), shape((4 * K, G), bf16)),
        (pltpu.VMEM((4 * MAXB, BLOCK), f32),),
        smem=1,
    )(counts, *planes, seen, mix, vcos, vsin, uvw, weights)
    other_adj = lax.ppermute(adj, "facet", partner)
    shares = call(share_kernel, shape((32, K, 2 * ROWS), bf16))(
        adj, other_adj, cos_a, sin_a, fcos[:32], fsin[:32], lift_t, lift_s
    )
    shares = lax.all_to_all(shares, "facet", 0, 0, axis_index_groups=groups, tiled=True)
    image = call(image_kernel, shape((ROWS, 2 * L), bf16))(shares, column)
    return (image[None], resid.reshape(1, 2, 2, VISITS))


def solution(mesh):
    placed = (
        P("stokes", "facet", None),
        P(),
        P("facet"),
        P(None, "facet", None),
        P(None, None, "facet", None),
        P("stokes", "facet", None, None),
    )
    return jax.shard_map(
        body,
        mesh=mesh,
        in_specs=placed,
        out_specs=(P("stokes", "facet", None), P("stokes", "facet", None, None)),
        check_vma=False,
    )
```

```python
import functools
import math

import jax
import jax.numpy as jnp
import numpy as np
from jax import lax
from jax.experimental import pallas as pl
from jax.experimental.pallas import tpu as pltpu
from jax.sharding import PartitionSpec as P

K = 64
G = 256
L = 8192
PERIOD = 2048
ROWS = 64
FACETS = 64
TOTAL = 4096
MAXB = 64
BLOCK = 128
VISITS = 8192
CHUNK = 512

f32 = jnp.float32
bf16 = jnp.bfloat16


@functools.cache
def tables():
    lpos = np.arange(PERIOD)[None, :]
    cpos = np.arange(K)[:, None]
    angle = 2.0 * np.pi * ((4 * cpos * (lpos - 16)) % L) / L
    column = np.concatenate([np.cos(angle), -np.sin(angle)], 0) / math.sqrt(L)
    upos = np.arange(G)[:, None]
    kpos = np.arange(K)[None, :]
    mpos = np.arange(K) - K // 2
    phase = (mpos[None, None, :] * (upos - 4 * kpos)[:, :, None]) % G
    interp = np.exp(2j * np.pi * phase / G).sum(2) / (2.0 * K)
    kernel_t = (interp * np.exp(2j * np.pi * (upos - 4 * kpos) / 512)).real.T
    dpos = np.arange(ROWS) - ROWS // 2
    lift = interp @ np.exp(-2j * np.pi * np.arange(K)[:, None] * dpos[None, :] / 1024)
    lift = lift * np.exp(-2j * np.pi * upos / 128) / math.sqrt(TOTAL)
    lift_t = np.concatenate([lift.real.T, lift.imag.T], 0)
    lift_s = np.concatenate([-lift.imag.T, lift.real.T], 0)
    return (
        column.astype(np.float32),
        kernel_t.astype(np.float32),
        lift_t.astype(np.float32),
        lift_s.astype(np.float32),
    )


def half_sign():
    lane = lax.broadcasted_iota(jnp.int32, (1, 2 * K), 1)
    return jnp.where(lane < K, 1.0, -1.0).astype(f32)


def swap(x):
    return pltpu.roll(x, K, 1)


def one_hot(cells):
    grid_pos = lax.broadcasted_iota(jnp.int32, (G, cells.shape[1]), 0)
    return jnp.where(grid_pos == cells, 1.0, 0.0).astype(bf16)


def nt_dot(a, b):
    return lax.dot_general(a, b, (((1,), (1,)), ((), ())), preferred_element_type=f32)


def column_kernel(strips_ref, column_ref, out_ref):
    parts = []
    for base in (0, L):
        folded = strips_ref[:, base : base + PERIOD].astype(f32)
        for turn in range(1, 4):
            start = base + turn * PERIOD
            folded = folded + strips_ref[:, start : start + PERIOD].astype(f32)
        parts.append(folded.astype(bf16))
    product = nt_dot(column_ref[...], jnp.concatenate(parts, 0))
    coeffs = (product[:K] - half_sign() * swap(product[K:])).astype(bf16)
    for q in range(32):
        out_ref[q] = coeffs


def turn(n, period):
    t = n.astype(f32) * (4.0 / period)
    q = jnp.floor(t + 0.5)
    x = (t - q) * (math.pi / 2)
    quarter = q.astype(jnp.int32) & 3
    y = x * x
    s = x * (1.0 + y * (-1.0 / 6 + y * (1.0 / 120 + y * (-1.0 / 5040 + y * (1.0 / 362880)))))
    c = 1.0 + y * (-0.5 + y * (1.0 / 24 + y * (-1.0 / 720 + y * (1.0 / 40320))))
    odd = (quarter & 1) == 1
    cosine = jnp.where(odd, s, c)
    sine = jnp.where(odd, c, s)
    cosine = jnp.where((quarter == 1) | (quarter == 2), -cosine, cosine)
    sine = jnp.where(quarter >= 2, sine, -sine)
    return cosine, sine


def prepare_kernel(
    here_ref, sub_ref, cells_ref, kernel_ref, mueller_ref, observed_ref,
    cos_ref, sin_ref, acos_ref, asin_ref, fcos_ref, fsin_ref, vcos_ref, vsin_ref, mix_ref,
    seen_ref, sent_ref, weights_ref, steps_ref, rows_ref,
):
    here, plane = here_ref[0], here_ref[1]
    core = here & 1
    step = lax.broadcasted_iota(jnp.int32, (32, 2 * ROWS), 0)
    lane = lax.broadcasted_iota(jnp.int32, (32, 2 * ROWS), 1) & (ROWS - 1)
    mine = (2 * step + core) * ROWS + lane
    other = (2 * step + 1 - core) * ROWS + lane
    for sub in range(2):
        offset = sub_ref[2 * here + sub]
        cosine, sine = turn((mine * offset) & (TOTAL - 1), TOTAL)
        cos_ref[sub * FACETS : sub * FACETS + 32, :] = cosine
        sin_ref[sub * FACETS : sub * FACETS + 32, :] = sine
        acos_ref[sub * 32 : sub * 32 + 32, :] = cosine
        asin_ref[sub * 32 : sub * 32 + 32, :] = sine
        cosine, sine = turn((other * offset) & (TOTAL - 1), TOTAL)
        cos_ref[sub * FACETS + 32 : (sub + 1) * FACETS, :] = cosine
        sin_ref[sub * FACETS + 32 : (sub + 1) * FACETS, :] = sine
        offset = sub_ref[2 * (here + 1 - 2 * core) + sub]
        cosine, sine = turn((mine * offset) & (TOTAL - 1), TOTAL)
        acos_ref[64 + sub * 32 : 96 + sub * 32, :] = cosine
        asin_ref[64 + sub * 32 : 96 + sub * 32, :] = sine
    step = lax.broadcasted_iota(jnp.int32, (32, G), 0)
    lane = lax.broadcasted_iota(jnp.int32, (32, G), 1)
    for side, facet in enumerate((2 * step + core, 2 * step + 1 - core)):
        cosine, sine = turn((facet * lane) & (FACETS - 1), FACETS)
        fcos_ref[side * 32 : side * 32 + 32, :] = cosine
        fsin_ref[side * 32 : side * 32 + 32, :] = sine
    for sub in range(2):
        for b in range(MAXB):
            lanes = slice(b * BLOCK, (b + 1) * BLOCK)
            steps_ref[sub * MAXB + b : sub * MAXB + b + 1, :] = (
                2 * cells_ref[2, sub : sub + 1, lanes] + cells_ref[1, sub : sub + 1, lanes]
            )
            for part in range(2):
                at = (2 * sub + part) * MAXB + b
                seen_ref[at : at + 1, :] = observed_ref[sub, part : part + 1, lanes]
    sent_ref[...] = seen_ref[...].astype(bf16)
    cosine, sine = turn(steps_ref[...] & (2 * G - 1), 2 * G)
    vcos_ref[...] = cosine
    vsin_ref[...] = -sine
    rows_ref[...] = jnp.zeros_like(rows_ref)
    for corr in range(4):
        for t in range(4):
            entry = mueller_ref[(plane + corr) & 3, (plane + t) & 3]
            at = 4 * corr + t
            rows_ref[at : at + 1, :] = jnp.concatenate([entry[0:1, :], entry[1:2, :]], 1)
    mix_ref[...] = jnp.transpose(rows_ref[...])
    for sub in range(2):

        def chunk(n, carry):
            at = pl.ds(pl.multiple_of(n * CHUNK, CHUNK), CHUNK)
            picked = jnp.dot(
                kernel_ref[...], one_hot(cells_ref[1, sub : sub + 1, at]), preferred_element_type=f32
            )
            weights_ref[sub, :, at] = picked.astype(bf16)
            return carry

        lax.fori_loop(0, VISITS // CHUNK, chunk, 0, unroll=2)


def facet_lift(cos_row, sin_row, lift_ref, lift_s_ref):
    return (cos_row * lift_ref[...] + sin_row * lift_s_ref[...]).astype(bf16)


def model_kernel(
    mine_ref, other_ref, cos_ref, sin_ref, fcos_ref, fsin_ref, lift_ref, lift_s_ref, cells_ref,
    weights_ref, out_ref, rows_ref, lifted_ref, samples_ref,
):
    sign = half_sign()
    rows_ref[...] = jnp.zeros_like(rows_ref)
    for side, source in enumerate((mine_ref, other_ref)):

        def pair(i, carry):
            lefts, rights = [], []
            for e in range(2):
                q = 2 * i + e
                p = side * 32 + q
                first = source[q].astype(f32)
                second = swap(first)
                rights.append(
                    facet_lift(fcos_ref[pl.ds(p, 1), :], fsin_ref[pl.ds(p, 1), :], lift_ref, lift_s_ref)
                )
                blocks = []
                for sub in range(2):
                    pr = cos_ref[pl.ds(sub * FACETS + p, 1), :]
                    pi = sin_ref[pl.ds(sub * FACETS + p, 1), :]
                    blocks.append((first * (pr * sign) - second * pi).astype(bf16))
                    blocks.append((second * pr + first * (pi * sign)).astype(bf16))
                lefts.append(jnp.concatenate(blocks, 0))
            left = jnp.concatenate(lefts, 1)
            right = jnp.concatenate(rights, 0)
            rows_ref[...] += jnp.dot(left, right, preferred_element_type=f32)
            return carry

        lax.fori_loop(0, 16, pair, 0, unroll=2)
    lifted_ref[...] = rows_ref[...].astype(bf16)
    per = CHUNK // BLOCK
    for sub in range(2):

        def chunk(n, carry):
            at = pl.ds(pl.multiple_of(n * CHUNK, CHUNK), CHUNK)
            picked = jnp.dot(
                lifted_ref[sub * 2 * K : (sub + 1) * 2 * K, :],
                one_hot(cells_ref[0, sub : sub + 1, at]),
                preferred_element_type=f32,
            )
            weight = weights_ref[sub, :, at].astype(f32)
            m_re = jnp.sum(picked[:K] * weight, 0, keepdims=True)
            m_im = jnp.sum(picked[K:] * weight, 0, keepdims=True)
            for b in range(per):
                lanes = slice(b * BLOCK, (b + 1) * BLOCK)
                samples_ref[pl.ds(2 * sub * MAXB + n * per + b, 1), :] = m_re[:, lanes]
                samples_ref[pl.ds((2 * sub + 1) * MAXB + n * per + b, 1), :] = m_im[:, lanes]
            return carry

        lax.fori_loop(0, VISITS // CHUNK, chunk, 0, unroll=2)
    out_ref[...] = samples_ref[...].astype(bf16)


def residual_kernel(
    counts_ref, a_ref, b_ref, c_ref, d_ref, oa_ref, ob_ref, oc_ref, od_ref, mix_ref, cos_ref, sin_ref, cells_ref, weights_ref,
    resid_ref, out_ref, back_ref,
):
    planes = (a_ref, b_ref, c_ref, d_ref)
    seen = (oa_ref, ob_ref, oc_ref, od_ref)
    block = lax.broadcasted_iota(jnp.int32, (MAXB, BLOCK), 0)
    for sub in range(2):
        live = block < counts_ref[sub]
        here = slice(sub * MAXB, (sub + 1) * MAXB)
        re = slice(2 * sub * MAXB, (2 * sub + 1) * MAXB)
        im = slice((2 * sub + 1) * MAXB, (2 * sub + 2) * MAXB)
        cosine, sine = cos_ref[here, :], sin_ref[here, :]
        s_re = [p[re, :].astype(f32) for p in planes]
        s_im = [p[im, :].astype(f32) for p in planes]
        back_re = jnp.zeros((MAXB, BLOCK), f32)
        back_im = jnp.zeros((MAXB, BLOCK), f32)
        for corr in range(4):
            mix = [mix_ref[here, 4 * corr + t : 4 * corr + t + 1] for t in range(4)]
            m_re = sum(m * s for m, s in zip(mix, s_re))
            m_im = sum(m * s for m, s in zip(mix, s_im))
            o_re = seen[corr][re, :].astype(f32)
            o_im = seen[corr][im, :].astype(f32)
            r_re = jnp.where(live, o_re - (m_re * cosine + m_im * sine), 0.0)
            r_im = jnp.where(live, o_im - (m_im * cosine - m_re * sine), 0.0)
            if corr == 0:
                resid_ref[re, :] = r_re
                resid_ref[im, :] = r_im
            back_re = back_re + mix[0] * r_re
            back_im = back_im + mix[0] * r_im
        back_ref[re, :] = back_re * cosine - back_im * sine
        back_ref[im, :] = back_im * cosine + back_re * sine
    per = CHUNK // BLOCK
    for sub in range(2):

        def chunk(n, total):
            at = pl.ds(pl.multiple_of(n * CHUNK, CHUNK), CHUNK)

            def row(part):
                base = (2 * sub + part) * MAXB + n * per
                return jnp.concatenate([back_ref[pl.ds(base + b, 1), :] for b in range(per)], 1)

            g_re, g_im = row(0), row(1)
            weight = weights_ref[sub, :, at].astype(f32)
            v_re = (g_re * weight).astype(bf16)
            v_im = (g_im * weight).astype(bf16)
            return total + nt_dot(one_hot(cells_ref[0, sub : sub + 1, at]), jnp.concatenate([v_re, v_im], 0))

        total = lax.fori_loop(0, VISITS // CHUNK, chunk, jnp.zeros((G, 2 * K), f32), unroll=2)
        out_ref[sub * 2 * K : (sub + 1) * 2 * K, :] = jnp.transpose(total).astype(bf16)


def share_kernel(
    mine_ref, other_ref, cos_ref, sin_ref, fcos_ref, fsin_ref, lift_ref, lift_s_ref, out_ref
):
    sign = half_sign()
    left = jnp.concatenate([mine_ref[...], other_ref[...]], 0)

    def pair(i, carry):
        rights = []
        for e in range(2):
            q = 2 * i + e
            rights.append(
                facet_lift(fcos_ref[pl.ds(q, 1), :], fsin_ref[pl.ds(q, 1), :], lift_ref, lift_s_ref)
            )
        product = nt_dot(left, jnp.concatenate(rights, 0))
        for e in range(2):
            q = 2 * i + e
            total = jnp.zeros((K, 2 * ROWS), f32)
            for sub in range(4):
                g_re = product[sub * 2 * K : sub * 2 * K + K, e * 128 : (e + 1) * 128]
                g_im = product[sub * 2 * K + K : (sub + 1) * 2 * K, e * 128 : (e + 1) * 128]
                g_re = g_re * sign
                pr = cos_ref[pl.ds(sub * 32 + q, 1), :]
                pi = sin_ref[pl.ds(sub * 32 + q, 1), :]
                total = total + (g_re + swap(g_im)) * pr + (swap(g_re) + g_im) * (pi * sign)
            out_ref[q] = total.astype(bf16)
        return carry

    lax.fori_loop(0, 16, pair, 0, unroll=2)


def image_kernel(shares_ref, column_ref, out_ref):
    total = shares_ref[0].astype(f32)
    for q in range(1, 32):
        total = total + shares_ref[q].astype(f32)
    total = total.astype(bf16).astype(f32)
    both = jnp.concatenate([total, half_sign() * swap(total)], 0)
    left = jnp.transpose(both).astype(bf16)
    image = (8.0 * jnp.dot(left, column_ref[...], preferred_element_type=f32)).astype(bf16)
    for turn in range(4):
        out_ref[:, turn * PERIOD : (turn + 1) * PERIOD] = image[:ROWS]
        out_ref[:, L + turn * PERIOD : L + (turn + 1) * PERIOD] = image[ROWS:]


def call(kernel, out_shape, scratch=(), smem=0, limit=16, flops=10**9):
    vmem = pl.BlockSpec(memory_space=pltpu.VMEM)

    def run(*args):
        specs = [pl.BlockSpec(memory_space=pltpu.SMEM)] * smem + [vmem] * (len(args) - smem)
        return pl.pallas_call(
            kernel,
            out_shape=out_shape,
            in_specs=specs,
            out_specs=jax.tree.map(lambda _: vmem, out_shape),
            scratch_shapes=list(scratch),
            cost_estimate=pl.CostEstimate(flops=flops, bytes_accessed=2**20, transcendentals=0),
            compiler_params=pltpu.CompilerParams(vmem_limit_bytes=limit * 2**20),
        )(*args)

    return run


def shape(dims, dtype):
    return jax.ShapeDtypeStruct(dims, dtype)


def body(strips, sub_u, counts, uvw, mueller, observed):
    column, kernel_t, lift_t, lift_s = tables()
    column = jnp.asarray(column, bf16)
    kernel_t = jnp.asarray(kernel_t, bf16)
    lift_t = jnp.asarray(lift_t)
    lift_s = jnp.asarray(lift_s)
    here = lax.axis_index("facet")
    plane = lax.axis_index("stokes")
    groups = [[2 * q + side for q in range(32)] for side in range(2)]
    partner = [(i, i ^ 1) for i in range(FACETS)]

    def to_stokes(array):
        return [array] + [
            lax.ppermute(array, "stokes", [(i, (i - k) % 4) for i in range(4)]) for k in (1, 2, 3)
        ]

    spread = call(column_kernel, shape((32, K, 2 * ROWS), bf16))(strips[0], column)
    mine = lax.all_to_all(spread, "facet", 0, 0, axis_index_groups=groups, tiled=True)
    square = shape((128, 128), f32)
    half = shape((FACETS, G), f32)
    cos_f, sin_f, cos_a, sin_a, fcos, fsin, vcos, vsin, mix, seen, sent, weights = call(
        prepare_kernel,
        (square, square, square, square, half, half, square, square, square)
        + (
            shape((4 * MAXB, BLOCK), f32),
            shape((4 * MAXB, BLOCK), bf16),
            shape((2, K, VISITS), bf16),
        ),
        (pltpu.VMEM((128, 128), jnp.int32), pltpu.VMEM((128, 128), f32)),
        smem=2,
        flops=10**10,
    )(jnp.stack([here, plane]), sub_u, uvw, kernel_t, mueller, observed[0])
    seen = [seen] + to_stokes(sent)[1:]
    mine, weights = lax.optimization_barrier((mine, weights))
    other = lax.ppermute(mine, "facet", partner)
    samples = call(
        model_kernel,
        shape((4 * MAXB, BLOCK), bf16),
        (
            pltpu.VMEM((4 * K, G), f32),
            pltpu.VMEM((4 * K, G), bf16),
            pltpu.VMEM((4 * MAXB, BLOCK), f32),
        ),
    )(mine, other, cos_f, sin_f, fcos, fsin, lift_t, lift_s, uvw, weights)
    resid, adj = call(
        residual_kernel,
        (shape((4 * MAXB, BLOCK), f32), shape((4 * K, G), bf16)),
        (pltpu.VMEM((4 * MAXB, BLOCK), f32),),
        smem=1,
    )(counts, *to_stokes(samples), *seen, mix, vcos, vsin, uvw, weights)
    other_adj = lax.ppermute(adj, "facet", partner)
    shares = call(share_kernel, shape((32, K, 2 * ROWS), bf16))(
        adj, other_adj, cos_a, sin_a, fcos, fsin, lift_t, lift_s
    )
    shares = lax.all_to_all(shares, "facet", 0, 0, axis_index_groups=groups, tiled=True)
    image = call(image_kernel, shape((ROWS, 2 * L), bf16))(shares, column)
    return (image[None], resid.reshape(1, 2, 2, VISITS))


def solution(mesh):
    placed = (
        P("stokes", "facet", None),
        P(),
        P("facet"),
        P(None, "facet", None),
        P(None, None, "facet", None),
        P("stokes", "facet", None, None),
    )
    return jax.shard_map(
        body,
        mesh=mesh,
        in_specs=placed,
        out_specs=(P("stokes", "facet", None), P("stokes", "facet", None, None)),
        check_vma=False,
    )
```

```python
import functools
import math

import jax
import jax.numpy as jnp
import numpy as np
from jax import lax
from jax.experimental import pallas as pl
from jax.experimental.pallas import tpu as pltpu
from jax.sharding import PartitionSpec as P


K = 64
G = 256
L = 8192
PERIOD = 2048
ROWS = 64
FACETS = 64
TOTAL = 4096
MAXB = 64
BLOCK = 128
VISITS = 8192
CHUNK = 512
GROUP = 4

f32 = jnp.float32
bf16 = jnp.bfloat16


@functools.cache
def tables():
    lpos = np.arange(PERIOD)[None, :]
    cpos = np.arange(K)[:, None]
    angle = 2.0 * np.pi * ((4 * cpos * (lpos - 16)) % L) / L
    column = np.concatenate([np.cos(angle), -np.sin(angle)], 0) / math.sqrt(L)
    upos = np.arange(G)[:, None]
    kpos = np.arange(K)[None, :]
    mpos = np.arange(K) - K // 2
    phase = (mpos[None, None, :] * (upos - 4 * kpos)[:, :, None]) % G
    interp = np.exp(2j * np.pi * phase / G).sum(2) / (2.0 * K)
    kernel_t = (interp * np.exp(2j * np.pi * (upos - 4 * kpos) / 512)).real.T
    dpos = np.arange(ROWS) - ROWS // 2
    lift = interp @ np.exp(-2j * np.pi * np.arange(K)[:, None] * dpos[None, :] / 1024)
    lift = lift * np.exp(-2j * np.pi * upos / 128) / math.sqrt(TOTAL)
    lift_t = np.concatenate([lift.real.T, lift.imag.T], 0)
    lift_s = np.concatenate([-lift.imag.T, lift.real.T], 0)
    return (
        column.astype(np.float32),
        kernel_t.astype(np.float32),
        lift_t.astype(np.float32),
        lift_s.astype(np.float32),
    )


def half_sign():
    lane = lax.broadcasted_iota(jnp.int32, (1, 2 * K), 1)
    return jnp.where(lane < K, 1.0, -1.0).astype(f32)


def swap(x):
    return pltpu.roll(x, K, 1)


def one_hot(cells):
    grid_pos = lax.broadcasted_iota(jnp.int32, (G, cells.shape[1]), 0)
    return jnp.where(grid_pos == cells, 1.0, 0.0).astype(bf16)


def nt_dot(a, b):
    return lax.dot_general(a, b, (((1,), (1,)), ((), ())), preferred_element_type=f32)


def column_kernel(strips_ref, column_ref, out_ref, strips_buf, column_buf, sems):
    copies = [
        pltpu.make_async_copy(
            strips_ref.at[:, pl.ds(i * PERIOD, PERIOD)], strips_buf.at[i], sems.at[i]
        )
        for i in range(8)
    ]
    table = pltpu.make_async_copy(column_ref, column_buf, sems.at[8])
    for copy in copies:
        copy.start()
    table.start()
    parts = []
    for part in range(2):
        copies[4 * part].wait()
        copies[4 * part + 1].wait()
        folded = strips_buf[4 * part].astype(f32) + strips_buf[4 * part + 1].astype(f32)
        copies[4 * part + 2].wait()
        copies[4 * part + 3].wait()
        folded = folded + strips_buf[4 * part + 2].astype(f32) + strips_buf[4 * part + 3].astype(f32)
        parts.append(folded.astype(bf16))
    table.wait()
    product = nt_dot(column_buf[...], jnp.concatenate(parts, 0))
    coeffs = (product[:K] - half_sign() * swap(product[K:])).astype(bf16)
    for q in range(32):
        out_ref[q] = coeffs


def turn(n, period):
    t = n.astype(f32) * (4.0 / period)
    q = jnp.floor(t + 0.5)
    x = (t - q) * (math.pi / 2)
    quarter = q.astype(jnp.int32) & 3
    y = x * x
    s = x * (1.0 + y * (-1.0 / 6 + y * (1.0 / 120 + y * (-1.0 / 5040 + y * (1.0 / 362880)))))
    c = 1.0 + y * (-0.5 + y * (1.0 / 24 + y * (-1.0 / 720 + y * (1.0 / 40320))))
    odd = (quarter & 1) == 1
    cosine = jnp.where(odd, s, c)
    sine = jnp.where(odd, c, s)
    cosine = jnp.where((quarter == 1) | (quarter == 2), -cosine, cosine)
    sine = jnp.where(quarter >= 2, sine, -sine)
    return cosine, sine


def prepare_kernel(
    here_ref, cells_ref, kernel_ref, mueller_ref, observed_ref, vcos_ref, vsin_ref, mix_ref, seen_ref,
    sent_ref, weights_ref, steps_ref, rows_ref,
):
    plane = here_ref[1]
    for sub in range(2):
        for b in range(MAXB):
            lanes = slice(b * BLOCK, (b + 1) * BLOCK)
            steps_ref[sub * MAXB + b : sub * MAXB + b + 1, :] = (
                2 * cells_ref[2, sub : sub + 1, lanes] + cells_ref[1, sub : sub + 1, lanes]
            )
            for part in range(2):
                at = (2 * sub + part) * MAXB + b
                seen_ref[at : at + 1, :] = observed_ref[sub, part : part + 1, lanes]
    sent_ref[...] = seen_ref[...].astype(bf16)
    cosine, sine = turn(steps_ref[...] & (2 * G - 1), 2 * G)
    vcos_ref[...] = cosine
    vsin_ref[...] = -sine
    rows_ref[...] = jnp.zeros_like(rows_ref)
    for corr in range(4):
        for t in range(4):
            entry = mueller_ref[(plane + corr) & 3, (plane + t) & 3]
            at = 4 * corr + t
            rows_ref[at : at + 1, :] = jnp.concatenate([entry[0:1, :], entry[1:2, :]], 1)
    for t in range(4):
        rows_ref[16 + t : 17 + t, :] = sum(
            rows_ref[4 * corr : 4 * corr + 1, :] * rows_ref[4 * corr + t : 4 * corr + t + 1, :]
            for corr in range(4)
        )
    mix_ref[...] = jnp.transpose(rows_ref[...])
    for sub in range(2):

        def chunk(n, carry):
            at = pl.ds(pl.multiple_of(n * CHUNK, CHUNK), CHUNK)
            picked = jnp.dot(
                kernel_ref[...], one_hot(cells_ref[1, sub : sub + 1, at]), preferred_element_type=f32
            )
            weights_ref[sub, :, at] = picked.astype(bf16)
            return carry

        lax.fori_loop(0, VISITS // CHUNK, chunk, 0, unroll=2)


def phases(offsets, parity, cos_ref, sin_ref, fcos_ref, fsin_ref):
    step = lax.broadcasted_iota(jnp.int32, (32, 2 * ROWS), 0)
    lane = lax.broadcasted_iota(jnp.int32, (32, 2 * ROWS), 1) & (ROWS - 1)
    rows = (2 * step + parity) * ROWS + lane
    for i, offset in enumerate(offsets):
        cosine, sine = turn((rows * offset) & (TOTAL - 1), TOTAL)
        cos_ref[32 * i : 32 * i + 32, :] = cosine
        sin_ref[32 * i : 32 * i + 32, :] = sine
    step = lax.broadcasted_iota(jnp.int32, (32, G), 0)
    lane = lax.broadcasted_iota(jnp.int32, (32, G), 1)
    cosine, sine = turn(((2 * step + parity) * lane) & (FACETS - 1), FACETS)
    fcos_ref[...] = cosine
    fsin_ref[...] = sine


def facet_lift(cos_row, sin_row, lift_ref, lift_s_ref):
    return (cos_row * lift_ref[...] + sin_row * lift_s_ref[...]).astype(bf16)


def lift(here_ref, sub_ref, side, source, lift_ref, lift_s_ref, total_ref, tables):
    cos_ref, sin_ref, fcos_ref, fsin_ref = tables
    here = here_ref[0]
    core = here & 1
    offsets = [sub_ref[2 * here + sub] for sub in range(2)]
    phases(offsets, core if side == 0 else 1 - core, *tables)
    sign = half_sign()

    def group(i, carry):
        lefts, rights = [], []
        for e in range(GROUP):
            q = GROUP * i + e
            first = source[q].astype(f32)
            second = swap(first)
            rights.append(
                facet_lift(fcos_ref[pl.ds(q, 1), :], fsin_ref[pl.ds(q, 1), :], lift_ref, lift_s_ref)
            )
            blocks = []
            for sub in range(2):
                pr = cos_ref[pl.ds(sub * 32 + q, 1), :]
                pi = sin_ref[pl.ds(sub * 32 + q, 1), :]
                blocks.append((first * (pr * sign) - second * pi).astype(bf16))
                blocks.append((second * pr + first * (pi * sign)).astype(bf16))
            lefts.append(jnp.concatenate(blocks, 0))
        left = jnp.concatenate(lefts, 1)
        right = jnp.concatenate(rights, 0)
        total_ref[...] += jnp.dot(left, right, preferred_element_type=f32)
        return carry

    lax.fori_loop(0, 32 // GROUP, group, 0)


def lift_kernel(here_ref, sub_ref, mine_ref, lift_ref, lift_s_ref, rows_ref, *tables):
    rows_ref[...] = jnp.zeros_like(rows_ref)
    lift(here_ref, sub_ref, 0, mine_ref, lift_ref, lift_s_ref, rows_ref, tables)


def model_kernel(
    here_ref, sub_ref, start_ref, other_ref, lift_ref, lift_s_ref, cells_ref, weights_ref,
    out_ref, rows_ref, lifted_ref, samples_ref, *tables
):
    rows_ref[...] = start_ref[...]
    lift(here_ref, sub_ref, 1, other_ref, lift_ref, lift_s_ref, rows_ref, tables)
    lifted_ref[...] = rows_ref[...].astype(bf16)
    per = CHUNK // BLOCK
    for sub in range(2):

        def chunk(n, carry):
            at = pl.ds(pl.multiple_of(n * CHUNK, CHUNK), CHUNK)
            picked = jnp.dot(
                lifted_ref[sub * 2 * K : (sub + 1) * 2 * K, :],
                one_hot(cells_ref[0, sub : sub + 1, at]),
                preferred_element_type=f32,
            )
            weight = weights_ref[sub, :, at].astype(f32)
            m_re = jnp.sum(picked[:K] * weight, 0, keepdims=True)
            m_im = jnp.sum(picked[K:] * weight, 0, keepdims=True)
            for b in range(per):
                lanes = slice(b * BLOCK, (b + 1) * BLOCK)
                samples_ref[pl.ds(2 * sub * MAXB + n * per + b, 1), :] = m_re[:, lanes]
                samples_ref[pl.ds((2 * sub + 1) * MAXB + n * per + b, 1), :] = m_im[:, lanes]
            return carry

        lax.fori_loop(0, VISITS // CHUNK, chunk, 0, unroll=2)
    out_ref[...] = samples_ref[...].astype(bf16)


def parts_of(sub):
    return (
        slice(sub * MAXB, (sub + 1) * MAXB),
        slice(2 * sub * MAXB, (2 * sub + 1) * MAXB),
        slice((2 * sub + 1) * MAXB, (2 * sub + 2) * MAXB),
    )


def observed_kernel(a_ref, b_ref, c_ref, d_ref, mix_ref, cos_ref, sin_ref, out_ref):
    for sub in range(2):
        here, re, im = parts_of(sub)
        cosine, sine = cos_ref[here, :], sin_ref[here, :]
        back_re = jnp.zeros((MAXB, BLOCK), f32)
        back_im = jnp.zeros((MAXB, BLOCK), f32)
        for corr, seen in enumerate((a_ref, b_ref, c_ref, d_ref)):
            mix = mix_ref[here, 4 * corr : 4 * corr + 1]
            back_re = back_re + mix * seen[re, :].astype(f32)
            back_im = back_im + mix * seen[im, :].astype(f32)
        out_ref[re, :] = back_re * cosine - back_im * sine
        out_ref[im, :] = back_im * cosine + back_re * sine


def residual_kernel(
    counts_ref, a_ref, b_ref, c_ref, d_ref, seen_ref, turned_ref, mix_ref, cos_ref, sin_ref, cells_ref,
    weights_ref, resid_ref, out_ref, back_ref,
):
    planes = (a_ref, b_ref, c_ref, d_ref)
    block = lax.broadcasted_iota(jnp.int32, (MAXB, BLOCK), 0)
    for sub in range(2):
        live = block < counts_ref[sub]
        here, re, im = parts_of(sub)
        cosine, sine = cos_ref[here, :], sin_ref[here, :]
        s_re = [p[re, :].astype(f32) for p in planes]
        s_im = [p[im, :].astype(f32) for p in planes]

        def mixed(first, samples):
            return sum(mix_ref[here, first + t : first + t + 1] * s for t, s in enumerate(samples))

        m_re, m_im = mixed(0, s_re), mixed(0, s_im)
        resid_ref[re, :] = jnp.where(live, seen_ref[re, :] - (m_re * cosine + m_im * sine), 0.0)
        resid_ref[im, :] = jnp.where(live, seen_ref[im, :] - (m_im * cosine - m_re * sine), 0.0)
        back_ref[re, :] = jnp.where(live, turned_ref[re, :] - mixed(16, s_re), 0.0)
        back_ref[im, :] = jnp.where(live, turned_ref[im, :] - mixed(16, s_im), 0.0)
    per = CHUNK // BLOCK
    for sub in range(2):

        def chunk(n, total):
            at = pl.ds(pl.multiple_of(n * CHUNK, CHUNK), CHUNK)

            def row(part):
                base = (2 * sub + part) * MAXB + n * per
                return jnp.concatenate([back_ref[pl.ds(base + b, 1), :] for b in range(per)], 1)

            g_re, g_im = row(0), row(1)
            weight = weights_ref[sub, :, at].astype(f32)
            v_re = (g_re * weight).astype(bf16)
            v_im = (g_im * weight).astype(bf16)
            return total + nt_dot(one_hot(cells_ref[0, sub : sub + 1, at]), jnp.concatenate([v_re, v_im], 0))

        total = lax.fori_loop(0, VISITS // CHUNK, chunk, jnp.zeros((G, 2 * K), f32), unroll=2)
        out_ref[sub * 2 * K : (sub + 1) * 2 * K, :] = jnp.transpose(total).astype(bf16)


def share_kernel(
    here_ref, sub_ref, mine_ref, other_ref, lift_ref, lift_s_ref, out_ref, *tables
):
    cos_ref, sin_ref, fcos_ref, fsin_ref = tables
    sign = half_sign()
    here = here_ref[0]
    core = here & 1
    firsts = (2 * here, 2 * (here + 1 - 2 * core))
    phases([sub_ref[first + sub] for first in firsts for sub in range(2)], core, *tables)
    left = jnp.concatenate([mine_ref[...], other_ref[...]], 0)

    def pair(i, carry):
        rights = []
        for e in range(2):
            q = 2 * i + e
            rights.append(
                facet_lift(fcos_ref[pl.ds(q, 1), :], fsin_ref[pl.ds(q, 1), :], lift_ref, lift_s_ref)
            )
        product = nt_dot(left, jnp.concatenate(rights, 0))
        for e in range(2):
            q = 2 * i + e
            total = jnp.zeros((K, 2 * ROWS), f32)
            swapped = jnp.zeros((K, 2 * ROWS), f32)
            for sub in range(4):
                g_re = product[sub * 2 * K : sub * 2 * K + K, e * 128 : (e + 1) * 128]
                g_im = product[sub * 2 * K + K : (sub + 1) * 2 * K, e * 128 : (e + 1) * 128]
                pr = cos_ref[pl.ds(sub * 32 + q, 1), :]
                pi = sin_ref[pl.ds(sub * 32 + q, 1), :]
                total = total + (g_re * pr + g_im * pi)
                swapped = swapped + (g_im * pr - g_re * pi)
            out_ref[q] = (total * sign + swap(swapped)).astype(bf16)
        return carry

    lax.fori_loop(0, 16, pair, 0, unroll=2)


def image_kernel(shares_ref, column_ref, out_ref):
    total = shares_ref[0].astype(f32)
    for q in range(1, 32):
        total = total + shares_ref[q].astype(f32)
    total = total.astype(bf16).astype(f32)
    both = jnp.concatenate([total, half_sign() * swap(total)], 0)
    left = jnp.transpose(both).astype(bf16)
    image = (8.0 * jnp.dot(left, column_ref[...], preferred_element_type=f32)).astype(bf16)
    for turn in range(4):
        out_ref[:, turn * PERIOD : (turn + 1) * PERIOD] = image[:ROWS]
        out_ref[:, L + turn * PERIOD : L + (turn + 1) * PERIOD] = image[ROWS:]


def call(kernel, out_shape, scratch=(), smem=0, limit=16, flops=10**9, hbm=False):
    vmem = pl.BlockSpec(memory_space=pltpu.VMEM)

    def run(*args):
        place = pl.BlockSpec(memory_space=pltpu.HBM) if hbm else vmem
        specs = [pl.BlockSpec(memory_space=pltpu.SMEM)] * smem + [place] * (len(args) - smem)
        return pl.pallas_call(
            kernel,
            out_shape=out_shape,
            in_specs=specs,
            out_specs=jax.tree.map(lambda _: vmem, out_shape),
            scratch_shapes=list(scratch),
            cost_estimate=pl.CostEstimate(flops=flops, bytes_accessed=2**20, transcendentals=0),
            compiler_params=pltpu.CompilerParams(vmem_limit_bytes=limit * 2**20),
        )(*args)

    return run


def shape(dims, dtype):
    return jax.ShapeDtypeStruct(dims, dtype)


def column_of_subgrids(strips, sub_u, counts, uvw, mueller, observed):
    column, kernel_t, lift_t, lift_s = tables()
    column = jnp.asarray(column, bf16)
    kernel_t = jnp.asarray(kernel_t, bf16)
    lift_t = jnp.asarray(lift_t)
    lift_s = jnp.asarray(lift_s)
    here = lax.axis_index("facet")
    plane = lax.axis_index("stokes")
    groups = [[2 * q + side for q in range(32)] for side in range(2)]
    partner = [(i, i ^ 1) for i in range(FACETS)]

    def to_stokes(array):
        out = [array]
        for k in (1, 2, 3):
            out.append(lax.ppermute(array, "stokes", [(i, (i - k) % 4) for i in range(4)]))
        return out

    spread = call(
        column_kernel,
        shape((32, K, 2 * ROWS), bf16),
        (
            pltpu.VMEM((8, ROWS, PERIOD), bf16),
            pltpu.VMEM((2 * K, PERIOD), bf16),
            pltpu.SemaphoreType.DMA((9,)),
        ),
        limit=60,
        hbm=True,
    )(strips[0], column)
    mine = lax.all_to_all(spread, "facet", 0, 0, axis_index_groups=groups, tiled=True)
    square = shape((128, 128), f32)
    position = jnp.stack([here, plane])
    vcos, vsin, mix, seen, sent, weights = call(
        prepare_kernel,
        (
            square,
            square,
            square,
            shape((4 * MAXB, BLOCK), f32),
            shape((4 * MAXB, BLOCK), bf16),
            shape((2, K, VISITS), bf16),
        ),
        (pltpu.VMEM((128, 128), jnp.int32), pltpu.VMEM((128, 128), f32)),
        smem=1,
        flops=10**10,
    )(position, uvw, kernel_t, mueller, observed[0])
    turned = call(observed_kernel, shape((4 * MAXB, BLOCK), f32))(
        seen, *to_stokes(sent)[1:], mix, vcos, vsin
    )
    other = lax.ppermute(mine, "facet", partner)

    def scratch(offsets):
        return tuple(
            pltpu.VMEM(dims, f32) for dims in ((32 * offsets, 128), (32 * offsets, 128), (32, G), (32, G))
        )

    rows = call(lift_kernel, shape((4 * K, G), f32), scratch(2), smem=2)(
        position, sub_u, mine, lift_t, lift_s
    )
    samples = call(
        model_kernel,
        shape((4 * MAXB, BLOCK), bf16),
        (
            pltpu.VMEM((4 * K, G), f32),
            pltpu.VMEM((4 * K, G), bf16),
            pltpu.VMEM((4 * MAXB, BLOCK), f32),
        )
        + scratch(2),
        smem=2,
    )(position, sub_u, rows, other, lift_t, lift_s, uvw, weights)
    resid, adj = call(
        residual_kernel,
        (shape((4 * MAXB, BLOCK), f32), shape((4 * K, G), bf16)),
        (pltpu.VMEM((4 * MAXB, BLOCK), f32),),
        smem=1,
    )(counts, *to_stokes(samples), seen, turned, mix, vcos, vsin, uvw, weights)
    other_adj = lax.ppermute(adj, "facet", partner)
    shares = call(share_kernel, shape((32, K, 2 * ROWS), bf16), scratch(4), smem=2)(
        position, sub_u, adj, other_adj, lift_t, lift_s
    )
    shares = lax.all_to_all(shares, "facet", 0, 0, axis_index_groups=groups, tiled=True)
    image = call(image_kernel, shape((ROWS, 2 * L), bf16))(shares, column)
    return (image[None], resid.reshape(1, 2, 2, VISITS))


def solution(mesh):
    placed = (
        P("stokes", "facet", None),
        P(),
        P("facet"),
        P(None, "facet", None),
        P(None, None, "facet", None),
        P("stokes", "facet", None, None),
    )
    return jax.shard_map(
        column_of_subgrids,
        mesh=mesh,
        in_specs=placed,
        out_specs=(P("stokes", "facet", None), P("stokes", "facet", None, None)),
        check_vma=False,
    )
```

```python
import functools
import math

import jax
import jax.numpy as jnp
import numpy as np
from jax import lax
from jax.experimental import pallas as pl
from jax.experimental.pallas import tpu as pltpu
from jax.sharding import PartitionSpec as P


K = 64
G = 256
L = 8192
PERIOD = 2048
ROWS = 64
FACETS = 64
TOTAL = 4096
MAXB = 64
BLOCK = 128
VISITS = 8192
CHUNK = 4096
GROUP = 16

f32 = jnp.float32
bf16 = jnp.bfloat16


@functools.cache
def tables():
    lpos = np.arange(PERIOD)[None, :]
    cpos = np.arange(K)[:, None]
    angle = 2.0 * np.pi * ((4 * cpos * (lpos - 16)) % L) / L
    column = np.concatenate([np.cos(angle), -np.sin(angle)], 0) / math.sqrt(L)
    upos = np.arange(G)[:, None]
    kpos = np.arange(K)[None, :]
    mpos = np.arange(K) - K // 2
    phase = (mpos[None, None, :] * (upos - 4 * kpos)[:, :, None]) % G
    interp = np.exp(2j * np.pi * phase / G).sum(2) / (2.0 * K)
    kernel_t = (interp * np.exp(2j * np.pi * (upos - 4 * kpos) / 512)).real.T
    dpos = np.arange(ROWS) - ROWS // 2
    lift = interp @ np.exp(-2j * np.pi * np.arange(K)[:, None] * dpos[None, :] / 1024)
    lift = lift * np.exp(-2j * np.pi * upos / 128) / math.sqrt(TOTAL)
    lift_t = np.concatenate([lift.real.T, lift.imag.T], 0)
    lift_s = np.concatenate([-lift.imag.T, lift.real.T], 0)
    return (
        column.astype(np.float32),
        kernel_t.astype(np.float32),
        lift_t.astype(np.float32),
        lift_s.astype(np.float32),
    )


def half_sign():
    lane = lax.broadcasted_iota(jnp.int32, (1, 2 * K), 1)
    return jnp.where(lane < K, 1.0, -1.0).astype(f32)


def swap(x):
    return pltpu.roll(x, K, 1)


def one_hot(cells):
    grid_pos = lax.broadcasted_iota(jnp.int32, (G, cells.shape[1]), 0)
    return jnp.where(grid_pos == cells, 1.0, 0.0).astype(bf16)


def nt_dot(a, b):
    return lax.dot_general(a, b, (((1,), (1,)), ((), ())), preferred_element_type=f32)


def column_kernel(strips_ref, column_ref, out_ref, strips_buf, column_buf, sems):
    copies = [
        pltpu.make_async_copy(
            strips_ref.at[:, pl.ds(i * PERIOD, PERIOD)], strips_buf.at[i], sems.at[i]
        )
        for i in range(8)
    ]
    table = pltpu.make_async_copy(column_ref, column_buf, sems.at[8])
    for copy in copies:
        copy.start()
    table.start()
    parts = []
    for part in range(2):
        copies[4 * part].wait()
        copies[4 * part + 1].wait()
        folded = strips_buf[4 * part].astype(f32) + strips_buf[4 * part + 1].astype(f32)
        copies[4 * part + 2].wait()
        copies[4 * part + 3].wait()
        folded = folded + strips_buf[4 * part + 2].astype(f32) + strips_buf[4 * part + 3].astype(f32)
        parts.append(folded.astype(bf16))
    table.wait()
    product = nt_dot(column_buf[...], jnp.concatenate(parts, 0))
    coeffs = (product[:K] - half_sign() * swap(product[K:])).astype(bf16)
    for q in range(32):
        out_ref[q] = coeffs


def turn(n, period):
    t = n.astype(f32) * (4.0 / period)
    q = jnp.floor(t + 0.5)
    x = (t - q) * (math.pi / 2)
    quarter = q.astype(jnp.int32) & 3
    y = x * x
    s = x * (1.0 + y * (-1.0 / 6 + y * (1.0 / 120 + y * (-1.0 / 5040 + y * (1.0 / 362880)))))
    c = 1.0 + y * (-0.5 + y * (1.0 / 24 + y * (-1.0 / 720 + y * (1.0 / 40320))))
    odd = (quarter & 1) == 1
    cosine = jnp.where(odd, s, c)
    sine = jnp.where(odd, c, s)
    cosine = jnp.where((quarter == 1) | (quarter == 2), -cosine, cosine)
    sine = jnp.where(quarter >= 2, sine, -sine)
    return cosine, sine


def prepare_kernel(
    here_ref, cells_ref, kernel_ref, mueller_ref, observed_ref, vcos_ref, vsin_ref, mix_ref, seen_ref,
    sent_ref, weights_ref, steps_ref, rows_ref,
):
    plane = here_ref[1]
    for sub in range(2):
        for b in range(MAXB):
            lanes = slice(b * BLOCK, (b + 1) * BLOCK)
            steps_ref[sub * MAXB + b : sub * MAXB + b + 1, :] = (
                2 * cells_ref[2, sub : sub + 1, lanes] + cells_ref[1, sub : sub + 1, lanes]
            )
            for part in range(2):
                at = (2 * sub + part) * MAXB + b
                seen_ref[at : at + 1, :] = observed_ref[sub, part : part + 1, lanes]
    sent_ref[...] = seen_ref[...].astype(bf16)
    cosine, sine = turn(steps_ref[...] & (2 * G - 1), 2 * G)
    vcos_ref[...] = cosine
    vsin_ref[...] = -sine
    rows_ref[...] = jnp.zeros_like(rows_ref)
    for corr in range(4):
        for t in range(4):
            entry = mueller_ref[(plane + corr) & 3, (plane + t) & 3]
            at = 4 * corr + t
            rows_ref[at : at + 1, :] = jnp.concatenate([entry[0:1, :], entry[1:2, :]], 1)
    for t in range(4):
        rows_ref[16 + t : 17 + t, :] = sum(
            rows_ref[4 * corr : 4 * corr + 1, :] * rows_ref[4 * corr + t : 4 * corr + t + 1, :]
            for corr in range(4)
        )
    mix_ref[...] = jnp.transpose(rows_ref[...])
    for sub in range(2):

        def chunk(n, carry):
            at = pl.ds(pl.multiple_of(n * CHUNK, CHUNK), CHUNK)
            picked = jnp.dot(
                kernel_ref[...], one_hot(cells_ref[1, sub : sub + 1, at]), preferred_element_type=f32
            )
            weights_ref[sub, :, at] = picked.astype(bf16)
            return carry

        lax.fori_loop(0, VISITS // CHUNK, chunk, 0, unroll=2)


def phases(offsets, parity, cos_ref, sin_ref, fcos_ref, fsin_ref):
    step = lax.broadcasted_iota(jnp.int32, (32, 2 * ROWS), 0)
    lane = lax.broadcasted_iota(jnp.int32, (32, 2 * ROWS), 1) & (ROWS - 1)
    rows = (2 * step + parity) * ROWS + lane
    for i, offset in enumerate(offsets):
        cosine, sine = turn((rows * offset) & (TOTAL - 1), TOTAL)
        cos_ref[32 * i : 32 * i + 32, :] = cosine
        sin_ref[32 * i : 32 * i + 32, :] = sine
    step = lax.broadcasted_iota(jnp.int32, (32, G), 0)
    lane = lax.broadcasted_iota(jnp.int32, (32, G), 1)
    cosine, sine = turn(((2 * step + parity) * lane) & (FACETS - 1), FACETS)
    fcos_ref[...] = cosine
    fsin_ref[...] = sine


def facet_lift(cos_row, sin_row, lift_ref, lift_s_ref):
    return (cos_row * lift_ref[...] + sin_row * lift_s_ref[...]).astype(bf16)


def lift(here_ref, sub_ref, side, source, lift_ref, lift_s_ref, total_ref, tables):
    cos_ref, sin_ref, fcos_ref, fsin_ref = tables
    here = here_ref[0]
    core = here & 1
    offsets = [sub_ref[2 * here + sub] for sub in range(2)]
    phases(offsets, core if side == 0 else 1 - core, *tables)
    sign = half_sign()

    def group(i, carry):
        lefts, rights = [], []
        for e in range(GROUP):
            q = GROUP * i + e
            first = source[q].astype(f32)
            second = swap(first)
            rights.append(
                facet_lift(fcos_ref[pl.ds(q, 1), :], fsin_ref[pl.ds(q, 1), :], lift_ref, lift_s_ref)
            )
            blocks = []
            for sub in range(2):
                pr = cos_ref[pl.ds(sub * 32 + q, 1), :]
                pi = sin_ref[pl.ds(sub * 32 + q, 1), :]
                blocks.append((first * (pr * sign) - second * pi).astype(bf16))
                blocks.append((second * pr + first * (pi * sign)).astype(bf16))
            lefts.append(jnp.concatenate(blocks, 0))
        left = jnp.concatenate(lefts, 1)
        right = jnp.concatenate(rights, 0)
        total_ref[...] += jnp.dot(left, right, preferred_element_type=f32)
        return carry

    lax.fori_loop(0, 32 // GROUP, group, 0)


def lift_kernel(here_ref, sub_ref, mine_ref, lift_ref, lift_s_ref, rows_ref, *tables):
    rows_ref[...] = jnp.zeros_like(rows_ref)
    lift(here_ref, sub_ref, 0, mine_ref, lift_ref, lift_s_ref, rows_ref, tables)


def model_kernel(
    here_ref, sub_ref, start_ref, other_ref, lift_ref, lift_s_ref, cells_ref, weights_ref,
    out_ref, rows_ref, lifted_ref, samples_ref, *tables
):
    rows_ref[...] = start_ref[...]
    lift(here_ref, sub_ref, 1, other_ref, lift_ref, lift_s_ref, rows_ref, tables)
    lifted_ref[...] = rows_ref[...].astype(bf16)
    per = CHUNK // BLOCK
    for sub in range(2):

        def chunk(n, carry):
            at = pl.ds(pl.multiple_of(n * CHUNK, CHUNK), CHUNK)
            picked = jnp.dot(
                lifted_ref[sub * 2 * K : (sub + 1) * 2 * K, :],
                one_hot(cells_ref[0, sub : sub + 1, at]),
                preferred_element_type=f32,
            )
            weight = weights_ref[sub, :, at].astype(f32)
            m_re = jnp.sum(picked[:K] * weight, 0, keepdims=True)
            m_im = jnp.sum(picked[K:] * weight, 0, keepdims=True)
            for b in range(per):
                lanes = slice(b * BLOCK, (b + 1) * BLOCK)
                samples_ref[pl.ds(2 * sub * MAXB + n * per + b, 1), :] = m_re[:, lanes]
                samples_ref[pl.ds((2 * sub + 1) * MAXB + n * per + b, 1), :] = m_im[:, lanes]
            return carry

        lax.fori_loop(0, VISITS // CHUNK, chunk, 0, unroll=2)
    out_ref[...] = samples_ref[...].astype(bf16)


def parts_of(sub):
    return (
        slice(sub * MAXB, (sub + 1) * MAXB),
        slice(2 * sub * MAXB, (2 * sub + 1) * MAXB),
        slice((2 * sub + 1) * MAXB, (2 * sub + 2) * MAXB),
    )


def observed_kernel(a_ref, b_ref, c_ref, d_ref, mix_ref, cos_ref, sin_ref, out_ref):
    for sub in range(2):
        here, re, im = parts_of(sub)
        cosine, sine = cos_ref[here, :], sin_ref[here, :]
        back_re = jnp.zeros((MAXB, BLOCK), f32)
        back_im = jnp.zeros((MAXB, BLOCK), f32)
        for corr, seen in enumerate((a_ref, b_ref, c_ref, d_ref)):
            mix = mix_ref[here, 4 * corr : 4 * corr + 1]
            back_re = back_re + mix * seen[re, :].astype(f32)
            back_im = back_im + mix * seen[im, :].astype(f32)
        out_ref[re, :] = back_re * cosine - back_im * sine
        out_ref[im, :] = back_im * cosine + back_re * sine


def residual_kernel(
    counts_ref, a_ref, b_ref, c_ref, d_ref, seen_ref, turned_ref, mix_ref, cos_ref, sin_ref, cells_ref,
    weights_ref, resid_ref, out_ref, back_ref,
):
    planes = (a_ref, b_ref, c_ref, d_ref)
    block = lax.broadcasted_iota(jnp.int32, (MAXB, BLOCK), 0)
    for sub in range(2):
        live = block < counts_ref[sub]
        here, re, im = parts_of(sub)
        cosine, sine = cos_ref[here, :], sin_ref[here, :]
        s_re = [p[re, :].astype(f32) for p in planes]
        s_im = [p[im, :].astype(f32) for p in planes]

        def mixed(first, samples):
            return sum(mix_ref[here, first + t : first + t + 1] * s for t, s in enumerate(samples))

        m_re, m_im = mixed(0, s_re), mixed(0, s_im)
        resid_ref[re, :] = jnp.where(live, seen_ref[re, :] - (m_re * cosine + m_im * sine), 0.0)
        resid_ref[im, :] = jnp.where(live, seen_ref[im, :] - (m_im * cosine - m_re * sine), 0.0)
        back_ref[re, :] = jnp.where(live, turned_ref[re, :] - mixed(16, s_re), 0.0)
        back_ref[im, :] = jnp.where(live, turned_ref[im, :] - mixed(16, s_im), 0.0)
    per = CHUNK // BLOCK
    for sub in range(2):

        def chunk(n, total):
            at = pl.ds(pl.multiple_of(n * CHUNK, CHUNK), CHUNK)

            def row(part):
                base = (2 * sub + part) * MAXB + n * per
                return jnp.concatenate([back_ref[pl.ds(base + b, 1), :] for b in range(per)], 1)

            g_re, g_im = row(0), row(1)
            weight = weights_ref[sub, :, at].astype(f32)
            v_re = (g_re * weight).astype(bf16)
            v_im = (g_im * weight).astype(bf16)
            return total + nt_dot(one_hot(cells_ref[0, sub : sub + 1, at]), jnp.concatenate([v_re, v_im], 0))

        total = lax.fori_loop(0, VISITS // CHUNK, chunk, jnp.zeros((G, 2 * K), f32), unroll=2)
        out_ref[sub * 2 * K : (sub + 1) * 2 * K, :] = jnp.transpose(total).astype(bf16)


def share_kernel(
    here_ref, sub_ref, mine_ref, other_ref, lift_ref, lift_s_ref, out_ref, *tables
):
    cos_ref, sin_ref, fcos_ref, fsin_ref = tables
    sign = half_sign()
    here = here_ref[0]
    core = here & 1
    firsts = (2 * here, 2 * (here + 1 - 2 * core))
    phases([sub_ref[first + sub] for first in firsts for sub in range(2)], core, *tables)
    left = jnp.concatenate([mine_ref[...], other_ref[...]], 0)

    def pair(i, carry):
        rights = []
        for e in range(2):
            q = 2 * i + e
            rights.append(
                facet_lift(fcos_ref[pl.ds(q, 1), :], fsin_ref[pl.ds(q, 1), :], lift_ref, lift_s_ref)
            )
        product = nt_dot(left, jnp.concatenate(rights, 0))
        for e in range(2):
            q = 2 * i + e
            total = jnp.zeros((K, 2 * ROWS), f32)
            swapped = jnp.zeros((K, 2 * ROWS), f32)
            for sub in range(4):
                g_re = product[sub * 2 * K : sub * 2 * K + K, e * 128 : (e + 1) * 128]
                g_im = product[sub * 2 * K + K : (sub + 1) * 2 * K, e * 128 : (e + 1) * 128]
                pr = cos_ref[pl.ds(sub * 32 + q, 1), :]
                pi = sin_ref[pl.ds(sub * 32 + q, 1), :]
                total = total + (g_re * pr + g_im * pi)
                swapped = swapped + (g_im * pr - g_re * pi)
            out_ref[q] = (total * sign + swap(swapped)).astype(bf16)
        return carry

    lax.fori_loop(0, 16, pair, 0, unroll=4)


def image_kernel(shares_ref, column_ref, out_ref):
    total = shares_ref[0].astype(f32)
    for q in range(1, 32):
        total = total + shares_ref[q].astype(f32)
    total = total.astype(bf16).astype(f32)
    both = jnp.concatenate([total, half_sign() * swap(total)], 0)
    left = jnp.transpose(both).astype(bf16)
    image = (8.0 * jnp.dot(left, column_ref[...], preferred_element_type=f32)).astype(bf16)
    for turn in range(4):
        out_ref[:, turn * PERIOD : (turn + 1) * PERIOD] = image[:ROWS]
        out_ref[:, L + turn * PERIOD : L + (turn + 1) * PERIOD] = image[ROWS:]


def call(kernel, out_shape, scratch=(), smem=0, limit=16, flops=10**9, hbm=False):
    vmem = pl.BlockSpec(memory_space=pltpu.VMEM)

    def run(*args):
        place = pl.BlockSpec(memory_space=pltpu.HBM) if hbm else vmem
        specs = [pl.BlockSpec(memory_space=pltpu.SMEM)] * smem + [place] * (len(args) - smem)
        return pl.pallas_call(
            kernel,
            out_shape=out_shape,
            in_specs=specs,
            out_specs=jax.tree.map(lambda _: vmem, out_shape),
            scratch_shapes=list(scratch),
            cost_estimate=pl.CostEstimate(flops=flops, bytes_accessed=2**20, transcendentals=0),
            compiler_params=pltpu.CompilerParams(vmem_limit_bytes=limit * 2**20),
        )(*args)

    return run


def shape(dims, dtype):
    return jax.ShapeDtypeStruct(dims, dtype)


def column_of_subgrids(strips, sub_u, counts, uvw, mueller, observed):
    column, kernel_t, lift_t, lift_s = tables()
    column = jnp.asarray(column, bf16)
    kernel_t = jnp.asarray(kernel_t, bf16)
    lift_t = jnp.asarray(lift_t)
    lift_s = jnp.asarray(lift_s)
    here = lax.axis_index("facet")
    plane = lax.axis_index("stokes")
    groups = [[2 * q + side for q in range(32)] for side in range(2)]
    partner = [(i, i ^ 1) for i in range(FACETS)]

    def to_stokes(array):
        out = [array]
        for k in (1, 2, 3):
            out.append(lax.ppermute(array, "stokes", [(i, (i - k) % 4) for i in range(4)]))
        return out

    spread = call(
        column_kernel,
        shape((32, K, 2 * ROWS), bf16),
        (
            pltpu.VMEM((8, ROWS, PERIOD), bf16),
            pltpu.VMEM((2 * K, PERIOD), bf16),
            pltpu.SemaphoreType.DMA((9,)),
        ),
        limit=60,
        hbm=True,
    )(strips[0], column)
    mine = lax.all_to_all(spread, "facet", 0, 0, axis_index_groups=groups, tiled=True)
    square = shape((128, 128), f32)
    position = jnp.stack([here, plane])
    vcos, vsin, mix, seen, sent, weights = call(
        prepare_kernel,
        (
            square,
            square,
            square,
            shape((4 * MAXB, BLOCK), f32),
            shape((4 * MAXB, BLOCK), bf16),
            shape((2, K, VISITS), bf16),
        ),
        (pltpu.VMEM((128, 128), jnp.int32), pltpu.VMEM((128, 128), f32)),
        smem=1,
        flops=10**10,
    )(position, uvw, kernel_t, mueller, observed[0])
    turned = call(observed_kernel, shape((4 * MAXB, BLOCK), f32))(
        seen, *to_stokes(sent)[1:], mix, vcos, vsin
    )
    other = lax.ppermute(mine, "facet", partner)

    def scratch(offsets):
        return tuple(
            pltpu.VMEM(dims, f32) for dims in ((32 * offsets, 128), (32 * offsets, 128), (32, G), (32, G))
        )

    rows = call(lift_kernel, shape((4 * K, G), f32), scratch(2), smem=2)(
        position, sub_u, mine, lift_t, lift_s
    )
    samples = call(
        model_kernel,
        shape((4 * MAXB, BLOCK), bf16),
        (
            pltpu.VMEM((4 * K, G), f32),
            pltpu.VMEM((4 * K, G), bf16),
            pltpu.VMEM((4 * MAXB, BLOCK), f32),
        )
        + scratch(2),
        smem=2,
    )(position, sub_u, rows, other, lift_t, lift_s, uvw, weights)
    resid, adj = call(
        residual_kernel,
        (shape((4 * MAXB, BLOCK), f32), shape((4 * K, G), bf16)),
        (pltpu.VMEM((4 * MAXB, BLOCK), f32),),
        smem=1,
    )(counts, *to_stokes(samples), seen, turned, mix, vcos, vsin, uvw, weights)
    other_adj = lax.ppermute(adj, "facet", partner)
    shares = call(share_kernel, shape((32, K, 2 * ROWS), bf16), scratch(4), smem=2)(
        position, sub_u, adj, other_adj, lift_t, lift_s
    )
    shares = lax.all_to_all(shares, "facet", 0, 0, axis_index_groups=groups, tiled=True)
    image = call(image_kernel, shape((ROWS, 2 * L), bf16))(shares, column)
    return (image[None], resid.reshape(1, 2, 2, VISITS))


def solution(mesh):
    placed = (
        P("stokes", "facet", None),
        P(),
        P("facet"),
        P(None, "facet", None),
        P(None, None, "facet", None),
        P("stokes", "facet", None, None),
    )
    return jax.shard_map(
        column_of_subgrids,
        mesh=mesh,
        in_specs=placed,
        out_specs=(P("stokes", "facet", None), P("stokes", "facet", None, None)),
        check_vma=False,
    )
```

```python
import functools
import math

import jax
import jax.numpy as jnp
import numpy as np
from jax import lax
from jax.experimental import pallas as pl
from jax.experimental.pallas import tpu as pltpu
from jax.sharding import PartitionSpec as P


K = 64
G = 256
L = 8192
PERIOD = 2048
ROWS = 64
FACETS = 64
TOTAL = 4096
MAXB = 64
BLOCK = 128
VISITS = 8192
CHUNK = 4096
GROUP = 16
PIECES = 4
PIECE = PERIOD // PIECES

f32 = jnp.float32
bf16 = jnp.bfloat16


@functools.cache
def tables():
    lpos = np.arange(PERIOD)[None, :]
    cpos = np.arange(K)[:, None]
    angle = 2.0 * np.pi * ((4 * cpos * (lpos - 16)) % L) / L
    column = np.concatenate([np.cos(angle), -np.sin(angle)], 0) / math.sqrt(L)
    upos = np.arange(G)[:, None]
    kpos = np.arange(K)[None, :]
    mpos = np.arange(K) - K // 2
    phase = (mpos[None, None, :] * (upos - 4 * kpos)[:, :, None]) % G
    interp = np.exp(2j * np.pi * phase / G).sum(2) / (2.0 * K)
    kernel_t = (interp * np.exp(2j * np.pi * (upos - 4 * kpos) / 512)).real.T
    dpos = np.arange(ROWS) - ROWS // 2
    lift = interp @ np.exp(-2j * np.pi * np.arange(K)[:, None] * dpos[None, :] / 1024)
    lift = lift * np.exp(-2j * np.pi * upos / 128) / math.sqrt(TOTAL)
    lift_t = np.concatenate([lift.real.T, lift.imag.T], 0)
    lift_s = np.concatenate([-lift.imag.T, lift.real.T], 0)
    return (
        column.astype(np.float32),
        kernel_t.astype(np.float32),
        lift_t.astype(np.float32),
        lift_s.astype(np.float32),
    )


def half_sign():
    lane = lax.broadcasted_iota(jnp.int32, (1, 2 * K), 1)
    return jnp.where(lane < K, 1.0, -1.0).astype(f32)


def swap(x):
    return pltpu.roll(x, K, 1)


def one_hot(cells):
    grid_pos = lax.broadcasted_iota(jnp.int32, (G, cells.shape[1]), 0)
    return jnp.where(grid_pos == cells, 1.0, 0.0).astype(bf16)


def nt_dot(a, b):
    return lax.dot_general(a, b, (((1,), (1,)), ((), ())), preferred_element_type=f32)


def column_kernel(strips_ref, column_ref, out_ref, strips_buf, column_buf, sems):
    copies = []
    for piece in range(PIECES):
        start = piece * PIECE
        group = [
            pltpu.make_async_copy(
                strips_ref.at[:, pl.ds(i * PERIOD + start, PIECE)], strips_buf.at[piece, i], sems.at[piece, i]
            )
            for i in range(8)
        ]
        group.append(
            pltpu.make_async_copy(
                column_ref.at[:, pl.ds(start, PIECE)], column_buf.at[piece], sems.at[piece, 8]
            )
        )
        for copy in group:
            copy.start()
        copies.append(group)
    product = jnp.zeros((2 * K, 2 * ROWS), f32)
    for piece in range(PIECES):
        for copy in copies[piece]:
            copy.wait()
        parts = [
            sum(strips_buf[piece, 4 * part + turn].astype(f32) for turn in range(4)).astype(bf16)
            for part in range(2)
        ]
        product = product + nt_dot(column_buf[piece], jnp.concatenate(parts, 0))
    coeffs = (product[:K] - half_sign() * swap(product[K:])).astype(bf16)
    for q in range(32):
        out_ref[q] = coeffs


def turn(n, period):
    t = n.astype(f32) * (4.0 / period)
    q = jnp.floor(t + 0.5)
    x = (t - q) * (math.pi / 2)
    quarter = q.astype(jnp.int32) & 3
    y = x * x
    s = x * (1.0 + y * (-1.0 / 6 + y * (1.0 / 120 + y * (-1.0 / 5040 + y * (1.0 / 362880)))))
    c = 1.0 + y * (-0.5 + y * (1.0 / 24 + y * (-1.0 / 720 + y * (1.0 / 40320))))
    odd = (quarter & 1) == 1
    cosine = jnp.where(odd, s, c)
    sine = jnp.where(odd, c, s)
    cosine = jnp.where((quarter == 1) | (quarter == 2), -cosine, cosine)
    sine = jnp.where(quarter >= 2, sine, -sine)
    return cosine, sine


def prepare_kernel(
    here_ref, cells_ref, kernel_ref, mueller_ref, observed_ref, vcos_ref, vsin_ref, mix_ref, seen_ref,
    sent_ref, weights_ref, steps_ref, rows_ref,
):
    plane = here_ref[1]
    for sub in range(2):
        for b in range(MAXB):
            lanes = slice(b * BLOCK, (b + 1) * BLOCK)
            steps_ref[sub * MAXB + b : sub * MAXB + b + 1, :] = (
                2 * cells_ref[2, sub : sub + 1, lanes] + cells_ref[1, sub : sub + 1, lanes]
            )
            for part in range(2):
                at = (2 * sub + part) * MAXB + b
                seen_ref[at : at + 1, :] = observed_ref[sub, part : part + 1, lanes]
    sent_ref[...] = seen_ref[...].astype(bf16)
    cosine, sine = turn(steps_ref[...] & (2 * G - 1), 2 * G)
    vcos_ref[...] = cosine
    vsin_ref[...] = -sine
    rows_ref[...] = jnp.zeros_like(rows_ref)
    for corr in range(4):
        for t in range(4):
            entry = mueller_ref[(plane + corr) & 3, (plane + t) & 3]
            at = 4 * corr + t
            rows_ref[at : at + 1, :] = jnp.concatenate([entry[0:1, :], entry[1:2, :]], 1)
    for t in range(4):
        rows_ref[16 + t : 17 + t, :] = sum(
            rows_ref[4 * corr : 4 * corr + 1, :] * rows_ref[4 * corr + t : 4 * corr + t + 1, :]
            for corr in range(4)
        )
    mix_ref[...] = jnp.transpose(rows_ref[...])
    for sub in range(2):

        def chunk(n, carry):
            at = pl.ds(pl.multiple_of(n * CHUNK, CHUNK), CHUNK)
            picked = jnp.dot(
                kernel_ref[...], one_hot(cells_ref[1, sub : sub + 1, at]), preferred_element_type=f32
            )
            weights_ref[sub, :, at] = picked.astype(bf16)
            return carry

        lax.fori_loop(0, VISITS // CHUNK, chunk, 0, unroll=2)


def phases(offsets, parity, cos_ref, sin_ref, fcos_ref, fsin_ref):
    step = lax.broadcasted_iota(jnp.int32, (32, 2 * ROWS), 0)
    lane = lax.broadcasted_iota(jnp.int32, (32, 2 * ROWS), 1) & (ROWS - 1)
    rows = (2 * step + parity) * ROWS + lane
    for i, offset in enumerate(offsets):
        cosine, sine = turn((rows * offset) & (TOTAL - 1), TOTAL)
        cos_ref[32 * i : 32 * i + 32, :] = cosine
        sin_ref[32 * i : 32 * i + 32, :] = sine
    step = lax.broadcasted_iota(jnp.int32, (32, G), 0)
    lane = lax.broadcasted_iota(jnp.int32, (32, G), 1)
    cosine, sine = turn(((2 * step + parity) * lane) & (FACETS - 1), FACETS)
    fcos_ref[...] = cosine
    fsin_ref[...] = sine


def facet_lift(cos_row, sin_row, lift_ref, lift_s_ref):
    return (cos_row * lift_ref[...] + sin_row * lift_s_ref[...]).astype(bf16)


def lift(here_ref, sub_ref, side, source, lift_ref, lift_s_ref, total_ref, tables):
    cos_ref, sin_ref, fcos_ref, fsin_ref = tables
    here = here_ref[0]
    core = here & 1
    offsets = [sub_ref[2 * here + sub] for sub in range(2)]
    phases(offsets, core if side == 0 else 1 - core, *tables)
    sign = half_sign()

    def group(i, carry):
        lefts, rights = [], []
        for e in range(GROUP):
            q = GROUP * i + e
            first = source[q].astype(f32)
            second = swap(first)
            rights.append(
                facet_lift(fcos_ref[pl.ds(q, 1), :], fsin_ref[pl.ds(q, 1), :], lift_ref, lift_s_ref)
            )
            blocks = []
            for sub in range(2):
                pr = cos_ref[pl.ds(sub * 32 + q, 1), :]
                pi = sin_ref[pl.ds(sub * 32 + q, 1), :]
                blocks.append((first * (pr * sign) - second * pi).astype(bf16))
                blocks.append((second * pr + first * (pi * sign)).astype(bf16))
            lefts.append(jnp.concatenate(blocks, 0))
        left = jnp.concatenate(lefts, 1)
        right = jnp.concatenate(rights, 0)
        total_ref[...] += jnp.dot(left, right, preferred_element_type=f32)
        return carry

    lax.fori_loop(0, 32 // GROUP, group, 0)


def lift_kernel(here_ref, sub_ref, mine_ref, lift_ref, lift_s_ref, rows_ref, *tables):
    rows_ref[...] = jnp.zeros_like(rows_ref)
    lift(here_ref, sub_ref, 0, mine_ref, lift_ref, lift_s_ref, rows_ref, tables)


def model_kernel(
    here_ref, sub_ref, start_ref, other_ref, lift_ref, lift_s_ref, cells_ref, weights_ref,
    out_ref, rows_ref, lifted_ref, samples_ref, *tables
):
    rows_ref[...] = start_ref[...]
    lift(here_ref, sub_ref, 1, other_ref, lift_ref, lift_s_ref, rows_ref, tables)
    lifted_ref[...] = rows_ref[...].astype(bf16)
    per = CHUNK // BLOCK
    for sub in range(2):

        def chunk(n, carry):
            at = pl.ds(pl.multiple_of(n * CHUNK, CHUNK), CHUNK)
            picked = jnp.dot(
                lifted_ref[sub * 2 * K : (sub + 1) * 2 * K, :],
                one_hot(cells_ref[0, sub : sub + 1, at]),
                preferred_element_type=f32,
            )
            weight = weights_ref[sub, :, at].astype(f32)
            m_re = jnp.sum(picked[:K] * weight, 0, keepdims=True)
            m_im = jnp.sum(picked[K:] * weight, 0, keepdims=True)
            for b in range(per):
                lanes = slice(b * BLOCK, (b + 1) * BLOCK)
                samples_ref[pl.ds(2 * sub * MAXB + n * per + b, 1), :] = m_re[:, lanes]
                samples_ref[pl.ds((2 * sub + 1) * MAXB + n * per + b, 1), :] = m_im[:, lanes]
            return carry

        lax.fori_loop(0, VISITS // CHUNK, chunk, 0, unroll=2)
    out_ref[...] = samples_ref[...].astype(bf16)


def parts_of(sub):
    return (
        slice(sub * MAXB, (sub + 1) * MAXB),
        slice(2 * sub * MAXB, (2 * sub + 1) * MAXB),
        slice((2 * sub + 1) * MAXB, (2 * sub + 2) * MAXB),
    )


def observed_kernel(a_ref, b_ref, c_ref, d_ref, mix_ref, cos_ref, sin_ref, out_ref):
    for sub in range(2):
        here, re, im = parts_of(sub)
        cosine, sine = cos_ref[here, :], sin_ref[here, :]
        back_re = jnp.zeros((MAXB, BLOCK), f32)
        back_im = jnp.zeros((MAXB, BLOCK), f32)
        for corr, seen in enumerate((a_ref, b_ref, c_ref, d_ref)):
            mix = mix_ref[here, 4 * corr : 4 * corr + 1]
            back_re = back_re + mix * seen[re, :].astype(f32)
            back_im = back_im + mix * seen[im, :].astype(f32)
        out_ref[re, :] = back_re * cosine - back_im * sine
        out_ref[im, :] = back_im * cosine + back_re * sine


def residual_kernel(
    counts_ref, a_ref, b_ref, c_ref, d_ref, seen_ref, turned_ref, mix_ref, cos_ref, sin_ref, cells_ref,
    weights_ref, resid_ref, out_ref, back_ref,
):
    planes = (a_ref, b_ref, c_ref, d_ref)
    block = lax.broadcasted_iota(jnp.int32, (MAXB, BLOCK), 0)
    for sub in range(2):
        live = block < counts_ref[sub]
        here, re, im = parts_of(sub)
        cosine, sine = cos_ref[here, :], sin_ref[here, :]
        s_re = [p[re, :].astype(f32) for p in planes]
        s_im = [p[im, :].astype(f32) for p in planes]

        def mixed(first, samples):
            return sum(mix_ref[here, first + t : first + t + 1] * s for t, s in enumerate(samples))

        m_re, m_im = mixed(0, s_re), mixed(0, s_im)
        left_re = jnp.where(live, seen_ref[re, :] - (m_re * cosine + m_im * sine), 0.0)
        left_im = jnp.where(live, seen_ref[im, :] - (m_im * cosine - m_re * sine), 0.0)
        for b in range(MAXB):
            lanes = slice(b * BLOCK, (b + 1) * BLOCK)
            resid_ref[sub, 0:1, lanes] = left_re[b : b + 1, :]
            resid_ref[sub, 1:2, lanes] = left_im[b : b + 1, :]
        back_ref[re, :] = jnp.where(live, turned_ref[re, :] - mixed(16, s_re), 0.0)
        back_ref[im, :] = jnp.where(live, turned_ref[im, :] - mixed(16, s_im), 0.0)
    per = CHUNK // BLOCK
    for sub in range(2):

        def chunk(n, total):
            at = pl.ds(pl.multiple_of(n * CHUNK, CHUNK), CHUNK)

            def row(part):
                base = (2 * sub + part) * MAXB + n * per
                return jnp.concatenate([back_ref[pl.ds(base + b, 1), :] for b in range(per)], 1)

            g_re, g_im = row(0), row(1)
            weight = weights_ref[sub, :, at].astype(f32)
            v_re = (g_re * weight).astype(bf16)
            v_im = (g_im * weight).astype(bf16)
            return total + nt_dot(one_hot(cells_ref[0, sub : sub + 1, at]), jnp.concatenate([v_re, v_im], 0))

        total = lax.fori_loop(0, VISITS // CHUNK, chunk, jnp.zeros((G, 2 * K), f32), unroll=2)
        out_ref[sub * 2 * K : (sub + 1) * 2 * K, :] = jnp.transpose(total).astype(bf16)


def share_kernel(
    here_ref, sub_ref, mine_ref, other_ref, lift_ref, lift_s_ref, out_ref, *tables
):
    cos_ref, sin_ref, fcos_ref, fsin_ref = tables
    sign = half_sign()
    here = here_ref[0]
    core = here & 1
    firsts = (2 * here, 2 * (here + 1 - 2 * core))
    phases([sub_ref[first + sub] for first in firsts for sub in range(2)], core, *tables)
    left = jnp.concatenate([mine_ref[...], other_ref[...]], 0)

    def pair(i, carry):
        rights = []
        for e in range(2):
            q = 2 * i + e
            rights.append(
                facet_lift(fcos_ref[pl.ds(q, 1), :], fsin_ref[pl.ds(q, 1), :], lift_ref, lift_s_ref)
            )
        product = nt_dot(left, jnp.concatenate(rights, 0))
        for e in range(2):
            q = 2 * i + e
            total = jnp.zeros((K, 2 * ROWS), f32)
            swapped = jnp.zeros((K, 2 * ROWS), f32)
            for sub in range(4):
                g_re = product[sub * 2 * K : sub * 2 * K + K, e * 128 : (e + 1) * 128]
                g_im = product[sub * 2 * K + K : (sub + 1) * 2 * K, e * 128 : (e + 1) * 128]
                pr = cos_ref[pl.ds(sub * 32 + q, 1), :]
                pi = sin_ref[pl.ds(sub * 32 + q, 1), :]
                total = total + (g_re * pr + g_im * pi)
                swapped = swapped + (g_im * pr - g_re * pi)
            out_ref[q] = (total * sign + swap(swapped)).astype(bf16)
        return carry

    lax.fori_loop(0, 16, pair, 0, unroll=4)


def image_kernel(shares_ref, column_ref, out_ref, image_buf, sems):
    total = shares_ref[0].astype(f32)
    for q in range(1, 32):
        total = total + shares_ref[q].astype(f32)
    total = total.astype(bf16).astype(f32)
    both = jnp.concatenate([total, half_sign() * swap(total)], 0)
    left = jnp.transpose(both).astype(bf16)
    copies = []
    for piece in range(PIECES):
        start = piece * PIECE
        image = jnp.dot(left, column_ref[:, start : start + PIECE], preferred_element_type=f32)
        image_buf[piece] = (8.0 * image).astype(bf16)
        for i in range(8):
            copy = pltpu.make_async_copy(
                image_buf.at[piece, pl.ds(i // 4 * ROWS, ROWS)],
                out_ref.at[:, pl.ds(i * PERIOD + start, PIECE)],
                sems.at[piece, i],
            )
            copy.start()
            copies.append(copy)
    for copy in copies:
        copy.wait()


def call(kernel, out_shape, scratch=(), smem=0, limit=16, flops=10**9, hbm=False, hbm_out=False):
    vmem = pl.BlockSpec(memory_space=pltpu.VMEM)

    def run(*args):
        place = pl.BlockSpec(memory_space=pltpu.HBM) if hbm else vmem
        specs = [pl.BlockSpec(memory_space=pltpu.SMEM)] * smem + [place] * (len(args) - smem)
        result = pl.BlockSpec(memory_space=pltpu.HBM) if hbm_out else vmem
        return pl.pallas_call(
            kernel,
            out_shape=out_shape,
            in_specs=specs,
            out_specs=jax.tree.map(lambda _: result, out_shape),
            scratch_shapes=list(scratch),
            cost_estimate=pl.CostEstimate(flops=flops, bytes_accessed=2**20, transcendentals=0),
            compiler_params=pltpu.CompilerParams(vmem_limit_bytes=limit * 2**20),
        )(*args)

    return run


def shape(dims, dtype):
    return jax.ShapeDtypeStruct(dims, dtype)


def column_of_subgrids(strips, sub_u, counts, uvw, mueller, observed):
    column, kernel_t, lift_t, lift_s = tables()
    column = jnp.asarray(column, bf16)
    kernel_t = jnp.asarray(kernel_t, bf16)
    lift_t = jnp.asarray(lift_t)
    lift_s = jnp.asarray(lift_s)
    here = lax.axis_index("facet")
    plane = lax.axis_index("stokes")
    groups = [[2 * q + side for q in range(32)] for side in range(2)]
    partner = [(i, i ^ 1) for i in range(FACETS)]

    def to_stokes(array):
        out = [array]
        for k in (1, 2, 3):
            out.append(lax.ppermute(array, "stokes", [(i, (i - k) % 4) for i in range(4)]))
        return out

    spread = call(
        column_kernel,
        shape((32, K, 2 * ROWS), bf16),
        (
            pltpu.VMEM((PIECES, 8, ROWS, PIECE), bf16),
            pltpu.VMEM((PIECES, 2 * K, PIECE), bf16),
            pltpu.SemaphoreType.DMA((PIECES, 9)),
        ),
        limit=60,
        hbm=True,
    )(strips[0], column)
    mine = lax.all_to_all(spread, "facet", 0, 0, axis_index_groups=groups, tiled=True)
    square = shape((128, 128), f32)
    position = jnp.stack([here, plane])
    vcos, vsin, mix, seen, sent, weights = call(
        prepare_kernel,
        (
            square,
            square,
            square,
            shape((4 * MAXB, BLOCK), f32),
            shape((4 * MAXB, BLOCK), bf16),
            shape((2, K, VISITS), bf16),
        ),
        (pltpu.VMEM((128, 128), jnp.int32), pltpu.VMEM((128, 128), f32)),
        smem=1,
        flops=10**10,
    )(position, uvw, kernel_t, mueller, observed[0])
    turned = call(observed_kernel, shape((4 * MAXB, BLOCK), f32))(
        seen, *to_stokes(sent)[1:], mix, vcos, vsin
    )
    other = lax.ppermute(mine, "facet", partner)

    def scratch(offsets):
        return tuple(
            pltpu.VMEM(dims, f32) for dims in ((32 * offsets, 128), (32 * offsets, 128), (32, G), (32, G))
        )

    rows = call(lift_kernel, shape((4 * K, G), f32), scratch(2), smem=2)(
        position, sub_u, mine, lift_t, lift_s
    )
    samples = call(
        model_kernel,
        shape((4 * MAXB, BLOCK), bf16),
        (
            pltpu.VMEM((4 * K, G), f32),
            pltpu.VMEM((4 * K, G), bf16),
            pltpu.VMEM((4 * MAXB, BLOCK), f32),
        )
        + scratch(2),
        smem=2,
    )(position, sub_u, rows, other, lift_t, lift_s, uvw, weights)
    resid, adj = call(
        residual_kernel,
        (shape((2, 2, VISITS), f32), shape((4 * K, G), bf16)),
        (pltpu.VMEM((4 * MAXB, BLOCK), f32),),
        smem=1,
    )(counts, *to_stokes(samples), seen, turned, mix, vcos, vsin, uvw, weights)
    other_adj = lax.ppermute(adj, "facet", partner)
    shares = call(share_kernel, shape((32, K, 2 * ROWS), bf16), scratch(4), smem=2)(
        position, sub_u, adj, other_adj, lift_t, lift_s
    )
    shares = lax.all_to_all(shares, "facet", 0, 0, axis_index_groups=groups, tiled=True)
    image = call(
        image_kernel,
        shape((ROWS, 2 * L), bf16),
        (pltpu.VMEM((PIECES, 2 * ROWS, PIECE), bf16), pltpu.SemaphoreType.DMA((PIECES, 8))),
        hbm_out=True,
    )(shares, column)
    return (image[None], resid[None])


def solution(mesh):
    placed = (
        P("stokes", "facet", None),
        P(),
        P("facet"),
        P(None, "facet", None),
        P(None, None, "facet", None),
        P("stokes", "facet", None, None),
    )
    return jax.shard_map(
        column_of_subgrids,
        mesh=mesh,
        in_specs=placed,
        out_specs=(P("stokes", "facet", None), P("stokes", "facet", None, None)),
        check_vma=False,
    )
```

```python
import functools
import math

import jax
import jax.numpy as jnp
import numpy as np
from jax import lax
from jax.experimental import pallas as pl
from jax.experimental.pallas import tpu as pltpu
from jax.sharding import PartitionSpec as P


K = 64
G = 256
L = 8192
PERIOD = 2048
ROWS = 64
FACETS = 64
TOTAL = 4096
MAXB = 64
BLOCK = 128
VISITS = 8192
CHUNK = 4096
GROUP = 16

f32 = jnp.float32
bf16 = jnp.bfloat16


@functools.cache
def tables():
    lpos = np.arange(PERIOD)[None, :]
    cpos = np.arange(K)[:, None]
    angle = 2.0 * np.pi * ((4 * cpos * (lpos - 16)) % L) / L
    column = np.concatenate([np.cos(angle), -np.sin(angle)], 0) / math.sqrt(L)
    upos = np.arange(G)[:, None]
    kpos = np.arange(K)[None, :]
    mpos = np.arange(K) - K // 2
    phase = (mpos[None, None, :] * (upos - 4 * kpos)[:, :, None]) % G
    interp = np.exp(2j * np.pi * phase / G).sum(2) / (2.0 * K)
    kernel_t = (interp * np.exp(2j * np.pi * (upos - 4 * kpos) / 512)).real.T
    dpos = np.arange(ROWS) - ROWS // 2
    lift = interp @ np.exp(-2j * np.pi * np.arange(K)[:, None] * dpos[None, :] / 1024)
    lift = lift * np.exp(-2j * np.pi * upos / 128) / math.sqrt(TOTAL)
    lift_t = np.concatenate([lift.real.T, lift.imag.T], 0)
    lift_s = np.concatenate([-lift.imag.T, lift.real.T], 0)
    return (
        column.astype(np.float32),
        kernel_t.astype(np.float32),
        lift_t.astype(np.float32),
        lift_s.astype(np.float32),
    )


def half_sign():
    lane = lax.broadcasted_iota(jnp.int32, (1, 2 * K), 1)
    return jnp.where(lane < K, 1.0, -1.0).astype(f32)


def swap(x):
    return pltpu.roll(x, K, 1)


def one_hot(cells):
    grid_pos = lax.broadcasted_iota(jnp.int32, (G, cells.shape[1]), 0)
    return jnp.where(grid_pos == cells, 1.0, 0.0).astype(bf16)


def nt_dot(a, b):
    return lax.dot_general(a, b, (((1,), (1,)), ((), ())), preferred_element_type=f32)


def column_kernel(strips_ref, column_ref, out_ref, strips_buf, column_buf, sems):
    copies = [
        pltpu.make_async_copy(
            strips_ref.at[:, pl.ds(i * PERIOD, PERIOD)], strips_buf.at[i], sems.at[i]
        )
        for i in range(8)
    ]
    table = pltpu.make_async_copy(column_ref, column_buf, sems.at[8])
    for copy in copies:
        copy.start()
    table.start()
    parts = []
    for part in range(2):
        copies[4 * part].wait()
        copies[4 * part + 1].wait()
        folded = strips_buf[4 * part].astype(f32) + strips_buf[4 * part + 1].astype(f32)
        copies[4 * part + 2].wait()
        copies[4 * part + 3].wait()
        folded = folded + strips_buf[4 * part + 2].astype(f32) + strips_buf[4 * part + 3].astype(f32)
        parts.append(folded.astype(bf16))
    table.wait()
    product = nt_dot(column_buf[...], jnp.concatenate(parts, 0))
    coeffs = (product[:K] - half_sign() * swap(product[K:])).astype(bf16)
    for q in range(32):
        out_ref[q] = coeffs


def turn(n, period):
    t = n.astype(f32) * (4.0 / period)
    q = jnp.floor(t + 0.5)
    x = (t - q) * (math.pi / 2)
    quarter = q.astype(jnp.int32) & 3
    y = x * x
    s = x * (1.0 + y * (-1.0 / 6 + y * (1.0 / 120 + y * (-1.0 / 5040 + y * (1.0 / 362880)))))
    c = 1.0 + y * (-0.5 + y * (1.0 / 24 + y * (-1.0 / 720 + y * (1.0 / 40320))))
    odd = (quarter & 1) == 1
    cosine = jnp.where(odd, s, c)
    sine = jnp.where(odd, c, s)
    cosine = jnp.where((quarter == 1) | (quarter == 2), -cosine, cosine)
    sine = jnp.where(quarter >= 2, sine, -sine)
    return cosine, sine


def prepare_kernel(
    here_ref, cells_ref, kernel_ref, mueller_ref, observed_ref, vcos_ref, vsin_ref, mix_ref, seen_ref,
    sent_ref, weights_ref, steps_ref, rows_ref,
):
    plane = here_ref[1]
    for sub in range(2):
        for b in range(MAXB):
            lanes = slice(b * BLOCK, (b + 1) * BLOCK)
            steps_ref[sub * MAXB + b : sub * MAXB + b + 1, :] = (
                2 * cells_ref[2, sub : sub + 1, lanes] + cells_ref[1, sub : sub + 1, lanes]
            )
            for part in range(2):
                at = (2 * sub + part) * MAXB + b
                seen_ref[at : at + 1, :] = observed_ref[sub, part : part + 1, lanes]
    sent_ref[...] = seen_ref[...].astype(bf16)
    cosine, sine = turn(steps_ref[...] & (2 * G - 1), 2 * G)
    vcos_ref[...] = cosine
    vsin_ref[...] = -sine
    rows_ref[...] = jnp.zeros_like(rows_ref)
    for corr in range(4):
        for t in range(4):
            entry = mueller_ref[(plane + corr) & 3, (plane + t) & 3]
            at = 4 * corr + t
            rows_ref[at : at + 1, :] = jnp.concatenate([entry[0:1, :], entry[1:2, :]], 1)
    for t in range(4):
        rows_ref[16 + t : 17 + t, :] = sum(
            rows_ref[4 * corr : 4 * corr + 1, :] * rows_ref[4 * corr + t : 4 * corr + t + 1, :]
            for corr in range(4)
        )
    mix_ref[...] = jnp.transpose(rows_ref[...])
    for sub in range(2):

        def chunk(n, carry):
            at = pl.ds(pl.multiple_of(n * CHUNK, CHUNK), CHUNK)
            picked = jnp.dot(
                kernel_ref[...], one_hot(cells_ref[1, sub : sub + 1, at]), preferred_element_type=f32
            )
            weights_ref[sub, :, at] = picked.astype(bf16)
            return carry

        lax.fori_loop(0, VISITS // CHUNK, chunk, 0, unroll=2)


def row_phases(offsets, parity, cos_ref, sin_ref):
    step = lax.broadcasted_iota(jnp.int32, (32, 2 * ROWS), 0)
    lane = lax.broadcasted_iota(jnp.int32, (32, 2 * ROWS), 1) & (ROWS - 1)
    rows = (2 * step + parity) * ROWS + lane
    for i, offset in enumerate(offsets):
        cosine, sine = turn((rows * offset) & (TOTAL - 1), TOTAL)
        cos_ref[32 * i : 32 * i + 32, :] = cosine
        sin_ref[32 * i : 32 * i + 32, :] = sine


def facet_phases(parity, fcos_ref, fsin_ref):
    step = lax.broadcasted_iota(jnp.int32, (32, G), 0)
    lane = lax.broadcasted_iota(jnp.int32, (32, G), 1)
    cosine, sine = turn(((2 * step + parity) * lane) & (FACETS - 1), FACETS)
    fcos_ref[...] = cosine
    fsin_ref[...] = sine


def facet_lift(cos_row, sin_row, lift_ref, lift_s_ref):
    return (cos_row * lift_ref[...] + sin_row * lift_s_ref[...]).astype(bf16)


def lift(here_ref, sub_ref, side, source, lift_ref, lift_s_ref, total_ref, tables):
    cos_ref, sin_ref, fcos_ref, fsin_ref = tables
    here = here_ref[0]
    core = here & 1
    offsets = [sub_ref[2 * here + sub] for sub in range(2)]
    parity = core if side == 0 else 1 - core
    row_phases(offsets, parity, cos_ref, sin_ref)
    facet_phases(parity, fcos_ref, fsin_ref)
    sign = half_sign()

    def group(i, carry):
        lefts, rights = [], []
        for e in range(GROUP):
            q = GROUP * i + e
            first = source[q].astype(f32)
            second = swap(first)
            rights.append(
                facet_lift(fcos_ref[pl.ds(q, 1), :], fsin_ref[pl.ds(q, 1), :], lift_ref, lift_s_ref)
            )
            blocks = []
            for sub in range(2):
                pr = cos_ref[pl.ds(sub * 32 + q, 1), :]
                pi = sin_ref[pl.ds(sub * 32 + q, 1), :]
                blocks.append((first * (pr * sign) - second * pi).astype(bf16))
                blocks.append((second * pr + first * (pi * sign)).astype(bf16))
            lefts.append(jnp.concatenate(blocks, 0))
        left = jnp.concatenate(lefts, 1)
        right = jnp.concatenate(rights, 0)
        total_ref[...] += jnp.dot(left, right, preferred_element_type=f32)
        return carry

    lax.fori_loop(0, 32 // GROUP, group, 0)


def lift_kernel(here_ref, sub_ref, mine_ref, lift_ref, lift_s_ref, rows_ref, *tables):
    rows_ref[...] = jnp.zeros_like(rows_ref)
    lift(here_ref, sub_ref, 0, mine_ref, lift_ref, lift_s_ref, rows_ref, tables)


def model_kernel(
    here_ref, sub_ref, start_ref, other_ref, lift_ref, lift_s_ref, cells_ref, weights_ref,
    out_ref, rows_ref, lifted_ref, samples_ref, *tables
):
    rows_ref[...] = start_ref[...]
    lift(here_ref, sub_ref, 1, other_ref, lift_ref, lift_s_ref, rows_ref, tables)
    lifted_ref[...] = rows_ref[...].astype(bf16)
    per = CHUNK // BLOCK
    for sub in range(2):

        def chunk(n, carry):
            at = pl.ds(pl.multiple_of(n * CHUNK, CHUNK), CHUNK)
            picked = jnp.dot(
                lifted_ref[sub * 2 * K : (sub + 1) * 2 * K, :],
                one_hot(cells_ref[0, sub : sub + 1, at]),
                preferred_element_type=f32,
            )
            weight = weights_ref[sub, :, at].astype(f32)
            m_re = jnp.sum(picked[:K] * weight, 0, keepdims=True)
            m_im = jnp.sum(picked[K:] * weight, 0, keepdims=True)
            for b in range(per):
                lanes = slice(b * BLOCK, (b + 1) * BLOCK)
                samples_ref[pl.ds(2 * sub * MAXB + n * per + b, 1), :] = m_re[:, lanes]
                samples_ref[pl.ds((2 * sub + 1) * MAXB + n * per + b, 1), :] = m_im[:, lanes]
            return carry

        lax.fori_loop(0, VISITS // CHUNK, chunk, 0, unroll=2)
    out_ref[...] = samples_ref[...].astype(bf16)


def parts_of(sub):
    return (
        slice(sub * MAXB, (sub + 1) * MAXB),
        slice(2 * sub * MAXB, (2 * sub + 1) * MAXB),
        slice((2 * sub + 1) * MAXB, (2 * sub + 2) * MAXB),
    )


def observed_kernel(a_ref, b_ref, c_ref, d_ref, mix_ref, cos_ref, sin_ref, out_ref):
    for sub in range(2):
        here, re, im = parts_of(sub)
        cosine, sine = cos_ref[here, :], sin_ref[here, :]
        back_re = jnp.zeros((MAXB, BLOCK), f32)
        back_im = jnp.zeros((MAXB, BLOCK), f32)
        for corr, seen in enumerate((a_ref, b_ref, c_ref, d_ref)):
            mix = mix_ref[here, 4 * corr : 4 * corr + 1]
            back_re = back_re + mix * seen[re, :].astype(f32)
            back_im = back_im + mix * seen[im, :].astype(f32)
        out_ref[re, :] = back_re * cosine - back_im * sine
        out_ref[im, :] = back_im * cosine + back_re * sine


def residual_kernel(
    counts_ref, a_ref, b_ref, c_ref, d_ref, seen_ref, turned_ref, mix_ref, cos_ref, sin_ref, cells_ref,
    weights_ref, final_ref, out_ref, back_ref, resid_ref, sem,
):
    planes = (a_ref, b_ref, c_ref, d_ref)
    block = lax.broadcasted_iota(jnp.int32, (MAXB, BLOCK), 0)
    for sub in range(2):
        live = block < counts_ref[sub]
        here, re, im = parts_of(sub)
        cosine, sine = cos_ref[here, :], sin_ref[here, :]
        s_re = [p[re, :].astype(f32) for p in planes]
        s_im = [p[im, :].astype(f32) for p in planes]

        def mixed(first, samples):
            return sum(mix_ref[here, first + t : first + t + 1] * s for t, s in enumerate(samples))

        m_re, m_im = mixed(0, s_re), mixed(0, s_im)
        left_re = jnp.where(live, seen_ref[re, :] - (m_re * cosine + m_im * sine), 0.0)
        left_im = jnp.where(live, seen_ref[im, :] - (m_im * cosine - m_re * sine), 0.0)
        for b in range(MAXB):
            lanes = slice(b * BLOCK, (b + 1) * BLOCK)
            resid_ref[sub, 0:1, lanes] = left_re[b : b + 1, :]
            resid_ref[sub, 1:2, lanes] = left_im[b : b + 1, :]
        back_ref[re, :] = jnp.where(live, turned_ref[re, :] - mixed(16, s_re), 0.0)
        back_ref[im, :] = jnp.where(live, turned_ref[im, :] - mixed(16, s_im), 0.0)
    finish = pltpu.make_async_copy(resid_ref, final_ref, sem)
    finish.start()
    per = CHUNK // BLOCK
    for sub in range(2):

        def chunk(n, total):
            at = pl.ds(pl.multiple_of(n * CHUNK, CHUNK), CHUNK)

            def row(part):
                base = (2 * sub + part) * MAXB + n * per
                return jnp.concatenate([back_ref[pl.ds(base + b, 1), :] for b in range(per)], 1)

            g_re, g_im = row(0), row(1)
            weight = weights_ref[sub, :, at].astype(f32)
            v_re = (g_re * weight).astype(bf16)
            v_im = (g_im * weight).astype(bf16)
            return total + nt_dot(one_hot(cells_ref[0, sub : sub + 1, at]), jnp.concatenate([v_re, v_im], 0))

        total = lax.fori_loop(0, VISITS // CHUNK, chunk, jnp.zeros((G, 2 * K), f32), unroll=2)
        out_ref[sub * 2 * K : (sub + 1) * 2 * K, :] = jnp.transpose(total).astype(bf16)
    finish.wait()


def table_kernel(here_ref, lift_ref, lift_s_ref, out_ref, fcos_ref, fsin_ref):
    facet_phases(here_ref[0] & 1, fcos_ref, fsin_ref)
    for q in range(32):
        out_ref[q * 2 * ROWS : (q + 1) * 2 * ROWS, :] = facet_lift(
            fcos_ref[q : q + 1, :], fsin_ref[q : q + 1, :], lift_ref, lift_s_ref
        )


def share_kernel(
    here_ref, sub_ref, mine_ref, other_ref, table_ref, out_ref, cos_ref, sin_ref
):
    sign = half_sign()
    here = here_ref[0]
    core = here & 1
    firsts = (2 * here, 2 * (here + 1 - 2 * core))
    row_phases([sub_ref[first + sub] for first in firsts for sub in range(2)], core, cos_ref, sin_ref)
    left = jnp.concatenate([mine_ref[...], other_ref[...]], 0)

    def pair(i, carry):
        at = pl.ds(pl.multiple_of(i * 4 * ROWS, 4 * ROWS), 4 * ROWS)
        product = nt_dot(left, table_ref[at, :])
        for e in range(2):
            q = 2 * i + e
            total = jnp.zeros((K, 2 * ROWS), f32)
            swapped = jnp.zeros((K, 2 * ROWS), f32)
            for sub in range(4):
                g_re = product[sub * 2 * K : sub * 2 * K + K, e * 128 : (e + 1) * 128]
                g_im = product[sub * 2 * K + K : (sub + 1) * 2 * K, e * 128 : (e + 1) * 128]
                pr = cos_ref[pl.ds(sub * 32 + q, 1), :]
                pi = sin_ref[pl.ds(sub * 32 + q, 1), :]
                total = total + (g_re * pr + g_im * pi)
                swapped = swapped + (g_im * pr - g_re * pi)
            out_ref[q] = (total * sign + swap(swapped)).astype(bf16)
        return carry

    lax.fori_loop(0, 16, pair, 0, unroll=4)


def image_kernel(shares_ref, column_ref, out_ref):
    total = shares_ref[0].astype(f32)
    for q in range(1, 32):
        total = total + shares_ref[q].astype(f32)
    total = total.astype(bf16).astype(f32)
    both = jnp.concatenate([total, half_sign() * swap(total)], 0)
    left = jnp.transpose(both).astype(bf16)
    image = (8.0 * jnp.dot(left, column_ref[...], preferred_element_type=f32)).astype(bf16)
    for turn in range(4):
        out_ref[:, turn * PERIOD : (turn + 1) * PERIOD] = image[:ROWS]
        out_ref[:, L + turn * PERIOD : L + (turn + 1) * PERIOD] = image[ROWS:]


def call(kernel, out_shape, scratch=(), smem=0, limit=16, flops=10**9, hbm=False, hbm_first=False):
    vmem = pl.BlockSpec(memory_space=pltpu.VMEM)

    def run(*args):
        place = pl.BlockSpec(memory_space=pltpu.HBM) if hbm else vmem
        specs = [pl.BlockSpec(memory_space=pltpu.SMEM)] * smem + [place] * (len(args) - smem)
        return pl.pallas_call(
            kernel,
            out_shape=out_shape,
            in_specs=specs,
            out_specs=(pl.BlockSpec(memory_space=pltpu.HBM), vmem)
            if hbm_first
            else jax.tree.map(lambda _: vmem, out_shape),
            scratch_shapes=list(scratch),
            cost_estimate=pl.CostEstimate(flops=flops, bytes_accessed=2**20, transcendentals=0),
            compiler_params=pltpu.CompilerParams(vmem_limit_bytes=limit * 2**20),
        )(*args)

    return run


def shape(dims, dtype):
    return jax.ShapeDtypeStruct(dims, dtype)


def column_of_subgrids(strips, sub_u, counts, uvw, mueller, observed):
    column, kernel_t, lift_t, lift_s = tables()
    column = jnp.asarray(column, bf16)
    kernel_t = jnp.asarray(kernel_t, bf16)
    lift_t = jnp.asarray(lift_t)
    lift_s = jnp.asarray(lift_s)
    here = lax.axis_index("facet")
    plane = lax.axis_index("stokes")
    groups = [[2 * q + side for q in range(32)] for side in range(2)]
    partner = [(i, i ^ 1) for i in range(FACETS)]

    def to_stokes(array):
        out = [array]
        for k in (1, 2, 3):
            out.append(lax.ppermute(array, "stokes", [(i, (i - k) % 4) for i in range(4)]))
        return out

    spread = call(
        column_kernel,
        shape((32, K, 2 * ROWS), bf16),
        (
            pltpu.VMEM((8, ROWS, PERIOD), bf16),
            pltpu.VMEM((2 * K, PERIOD), bf16),
            pltpu.SemaphoreType.DMA((9,)),
        ),
        limit=60,
        hbm=True,
    )(strips[0], column)
    mine = lax.all_to_all(spread, "facet", 0, 0, axis_index_groups=groups, tiled=True)
    square = shape((128, 128), f32)
    position = jnp.stack([here, plane])
    vcos, vsin, mix, seen, sent, weights = call(
        prepare_kernel,
        (
            square,
            square,
            square,
            shape((4 * MAXB, BLOCK), f32),
            shape((4 * MAXB, BLOCK), bf16),
            shape((2, K, VISITS), bf16),
        ),
        (pltpu.VMEM((128, 128), jnp.int32), pltpu.VMEM((128, 128), f32)),
        smem=1,
        flops=10**10,
    )(position, uvw, kernel_t, mueller, observed[0])
    turned = call(observed_kernel, shape((4 * MAXB, BLOCK), f32))(
        seen, *to_stokes(sent)[1:], mix, vcos, vsin
    )
    other = lax.ppermute(mine, "facet", partner)

    def scratch(offsets):
        return tuple(
            pltpu.VMEM(dims, f32) for dims in ((32 * offsets, 128), (32 * offsets, 128), (32, G), (32, G))
        )

    rows = call(lift_kernel, shape((4 * K, G), f32), scratch(2), smem=2)(
        position, sub_u, mine, lift_t, lift_s
    )
    samples = call(
        model_kernel,
        shape((4 * MAXB, BLOCK), bf16),
        (
            pltpu.VMEM((4 * K, G), f32),
            pltpu.VMEM((4 * K, G), bf16),
            pltpu.VMEM((4 * MAXB, BLOCK), f32),
        )
        + scratch(2),
        smem=2,
    )(position, sub_u, rows, other, lift_t, lift_s, uvw, weights)
    table = call(table_kernel, shape((64 * ROWS, G), bf16), scratch(0)[2:], smem=1)(
        position, lift_t, lift_s
    )
    resid, adj = call(
        residual_kernel,
        (shape((2, 2, VISITS), f32), shape((4 * K, G), bf16)),
        (
            pltpu.VMEM((4 * MAXB, BLOCK), f32),
            pltpu.VMEM((2, 2, VISITS), f32),
            pltpu.SemaphoreType.DMA(()),
        ),
        smem=1,
        hbm_first=True,
    )(counts, *to_stokes(samples), seen, turned, mix, vcos, vsin, uvw, weights)
    other_adj = lax.ppermute(adj, "facet", partner)
    shares = call(share_kernel, shape((32, K, 2 * ROWS), bf16), scratch(4)[:2], smem=2)(
        position, sub_u, adj, other_adj, table
    )
    shares = lax.all_to_all(shares, "facet", 0, 0, axis_index_groups=groups, tiled=True)
    image = call(image_kernel, shape((ROWS, 2 * L), bf16))(shares, column)
    return (image[None], resid[None])


def solution(mesh):
    placed = (
        P("stokes", "facet", None),
        P(),
        P("facet"),
        P(None, "facet", None),
        P(None, None, "facet", None),
        P("stokes", "facet", None, None),
    )
    return jax.shard_map(
        column_of_subgrids,
        mesh=mesh,
        in_specs=placed,
        out_specs=(P("stokes", "facet", None), P("stokes", "facet", None, None)),
        check_vma=False,
    )
```

```python
import functools
import math

import jax
import jax.numpy as jnp
import numpy as np
from jax import lax
from jax.experimental import pallas as pl
from jax.experimental.pallas import tpu as pltpu
from jax.sharding import PartitionSpec as P


K = 64
G = 256
L = 8192
PERIOD = 2048
ROWS = 64
FACETS = 64
TOTAL = 4096
MAXB = 64
BLOCK = 128
VISITS = 8192
CHUNK = 4096
GROUP = 16

f32 = jnp.float32
bf16 = jnp.bfloat16


@functools.cache
def tables():
    lpos = np.arange(PERIOD)[None, :]
    cpos = np.arange(K)[:, None]
    angle = 2.0 * np.pi * ((4 * cpos * (lpos - 16)) % L) / L
    column = np.concatenate([np.cos(angle), -np.sin(angle)], 0) / math.sqrt(L)
    upos = np.arange(G)[:, None]
    kpos = np.arange(K)[None, :]
    mpos = np.arange(K) - K // 2
    phase = (mpos[None, None, :] * (upos - 4 * kpos)[:, :, None]) % G
    interp = np.exp(2j * np.pi * phase / G).sum(2) / (2.0 * K)
    kernel_t = (interp * np.exp(2j * np.pi * (upos - 4 * kpos) / 512)).real.T
    dpos = np.arange(ROWS) - ROWS // 2
    lift = interp @ np.exp(-2j * np.pi * np.arange(K)[:, None] * dpos[None, :] / 1024)
    lift = lift * np.exp(-2j * np.pi * upos / 128) / math.sqrt(TOTAL)
    lift_t = np.concatenate([lift.real.T, lift.imag.T], 0)
    lift_s = np.concatenate([-lift.imag.T, lift.real.T], 0)
    return (
        column.astype(np.float32),
        kernel_t.astype(np.float32),
        lift_t.astype(np.float32),
        lift_s.astype(np.float32),
    )


def half_sign():
    lane = lax.broadcasted_iota(jnp.int32, (1, 2 * K), 1)
    return jnp.where(lane < K, 1.0, -1.0).astype(f32)


def swap(x):
    return pltpu.roll(x, K, 1)


def one_hot(cells):
    grid_pos = lax.broadcasted_iota(jnp.int32, (G, cells.shape[1]), 0)
    return jnp.where(grid_pos == cells, 1.0, 0.0).astype(bf16)


def nt_dot(a, b):
    return lax.dot_general(a, b, (((1,), (1,)), ((), ())), preferred_element_type=f32)


def column_kernel(strips_ref, column_ref, out_ref, strips_buf, column_buf, sems):
    copies = [
        pltpu.make_async_copy(
            strips_ref.at[:, pl.ds(i * PERIOD, PERIOD)], strips_buf.at[i], sems.at[i]
        )
        for i in range(8)
    ]
    table = pltpu.make_async_copy(column_ref, column_buf, sems.at[8])
    for copy in copies:
        copy.start()
    table.start()
    parts = []
    for part in range(2):
        copies[4 * part].wait()
        copies[4 * part + 1].wait()
        folded = strips_buf[4 * part].astype(f32) + strips_buf[4 * part + 1].astype(f32)
        copies[4 * part + 2].wait()
        copies[4 * part + 3].wait()
        folded = folded + strips_buf[4 * part + 2].astype(f32) + strips_buf[4 * part + 3].astype(f32)
        parts.append(folded.astype(bf16))
    table.wait()
    product = nt_dot(column_buf[...], jnp.concatenate(parts, 0))
    coeffs = (product[:K] - half_sign() * swap(product[K:])).astype(bf16)
    for q in range(32):
        out_ref[q] = coeffs


def turn(n, period):
    t = n.astype(f32) * (4.0 / period)
    q = jnp.floor(t + 0.5)
    x = (t - q) * (math.pi / 2)
    quarter = q.astype(jnp.int32) & 3
    y = x * x
    s = x * (1.0 + y * (-1.0 / 6 + y * (1.0 / 120 + y * (-1.0 / 5040 + y * (1.0 / 362880)))))
    c = 1.0 + y * (-0.5 + y * (1.0 / 24 + y * (-1.0 / 720 + y * (1.0 / 40320))))
    odd = (quarter & 1) == 1
    cosine = jnp.where(odd, s, c)
    sine = jnp.where(odd, c, s)
    cosine = jnp.where((quarter == 1) | (quarter == 2), -cosine, cosine)
    sine = jnp.where(quarter >= 2, sine, -sine)
    return cosine, sine


def prepare_kernel(
    here_ref, cells_ref, kernel_ref, mueller_ref, observed_ref, vcos_ref, vsin_ref, mix_ref, seen_ref,
    sent_ref, weights_ref, steps_ref, rows_ref,
):
    plane = here_ref[1]
    for sub in range(2):
        for b in range(MAXB):
            lanes = slice(b * BLOCK, (b + 1) * BLOCK)
            steps_ref[sub * MAXB + b : sub * MAXB + b + 1, :] = (
                2 * cells_ref[2, sub : sub + 1, lanes] + cells_ref[1, sub : sub + 1, lanes]
            )
            for part in range(2):
                at = (2 * sub + part) * MAXB + b
                seen_ref[at : at + 1, :] = observed_ref[sub, part : part + 1, lanes]
    sent_ref[...] = seen_ref[...].astype(bf16)
    cosine, sine = turn(steps_ref[...] & (2 * G - 1), 2 * G)
    vcos_ref[...] = cosine
    vsin_ref[...] = -sine
    rows_ref[...] = jnp.zeros_like(rows_ref)
    for corr in range(4):
        for t in range(4):
            entry = mueller_ref[(plane + corr) & 3, (plane + t) & 3]
            at = 4 * corr + t
            rows_ref[at : at + 1, :] = jnp.concatenate([entry[0:1, :], entry[1:2, :]], 1)
    for t in range(4):
        rows_ref[16 + t : 17 + t, :] = sum(
            rows_ref[4 * corr : 4 * corr + 1, :] * rows_ref[4 * corr + t : 4 * corr + t + 1, :]
            for corr in range(4)
        )
    mix_ref[...] = jnp.transpose(rows_ref[...])
    for sub in range(2):

        def chunk(n, carry):
            at = pl.ds(pl.multiple_of(n * CHUNK, CHUNK), CHUNK)
            picked = jnp.dot(
                kernel_ref[...], one_hot(cells_ref[1, sub : sub + 1, at]), preferred_element_type=f32
            )
            weights_ref[sub, :, at] = picked.astype(bf16)
            return carry

        lax.fori_loop(0, VISITS // CHUNK, chunk, 0, unroll=2)


def phases(offsets, parity, cos_ref, sin_ref, fcos_ref, fsin_ref):
    step = lax.broadcasted_iota(jnp.int32, (32, 2 * ROWS), 0)
    lane = lax.broadcasted_iota(jnp.int32, (32, 2 * ROWS), 1) & (ROWS - 1)
    rows = (2 * step + parity) * ROWS + lane
    for i, offset in enumerate(offsets):
        cosine, sine = turn((rows * offset) & (TOTAL - 1), TOTAL)
        cos_ref[32 * i : 32 * i + 32, :] = cosine
        sin_ref[32 * i : 32 * i + 32, :] = sine
    step = lax.broadcasted_iota(jnp.int32, (32, G), 0)
    lane = lax.broadcasted_iota(jnp.int32, (32, G), 1)
    cosine, sine = turn(((2 * step + parity) * lane) & (FACETS - 1), FACETS)
    fcos_ref[...] = cosine
    fsin_ref[...] = sine


def facet_lift(cos_row, sin_row, lift_ref, lift_s_ref):
    return (cos_row * lift_ref[...] + sin_row * lift_s_ref[...]).astype(bf16)


def lift(here_ref, sub_ref, side, source, lift_ref, lift_s_ref, total_ref, tables):
    cos_ref, sin_ref, fcos_ref, fsin_ref = tables
    here = here_ref[0]
    core = here & 1
    offsets = [sub_ref[2 * here + sub] for sub in range(2)]
    phases(offsets, core if side == 0 else 1 - core, *tables)
    sign = half_sign()

    def group(i, carry):
        lefts, rights = [], []
        for e in range(GROUP):
            q = GROUP * i + e
            first = source[q].astype(f32)
            second = swap(first)
            rights.append(
                facet_lift(fcos_ref[pl.ds(q, 1), :], fsin_ref[pl.ds(q, 1), :], lift_ref, lift_s_ref)
            )
            blocks = []
            for sub in range(2):
                pr = cos_ref[pl.ds(sub * 32 + q, 1), :]
                pi = sin_ref[pl.ds(sub * 32 + q, 1), :]
                blocks.append((first * (pr * sign) - second * pi).astype(bf16))
                blocks.append((second * pr + first * (pi * sign)).astype(bf16))
            lefts.append(jnp.concatenate(blocks, 0))
        left = jnp.concatenate(lefts, 1)
        right = jnp.concatenate(rights, 0)
        total_ref[...] += jnp.dot(left, right, preferred_element_type=f32)
        return carry

    lax.fori_loop(0, 32 // GROUP, group, 0)


def lift_kernel(here_ref, sub_ref, mine_ref, lift_ref, lift_s_ref, rows_ref, *tables):
    rows_ref[...] = jnp.zeros_like(rows_ref)
    lift(here_ref, sub_ref, 0, mine_ref, lift_ref, lift_s_ref, rows_ref, tables)


def model_kernel(
    here_ref, sub_ref, start_ref, other_ref, lift_ref, lift_s_ref, cells_ref, weights_ref,
    out_ref, rows_ref, lifted_ref, samples_ref, *tables
):
    rows_ref[...] = start_ref[...]
    lift(here_ref, sub_ref, 1, other_ref, lift_ref, lift_s_ref, rows_ref, tables)
    lifted_ref[...] = rows_ref[...].astype(bf16)
    per = CHUNK // BLOCK
    for sub in range(2):

        def chunk(n, carry):
            at = pl.ds(pl.multiple_of(n * CHUNK, CHUNK), CHUNK)
            picked = jnp.dot(
                lifted_ref[sub * 2 * K : (sub + 1) * 2 * K, :],
                one_hot(cells_ref[0, sub : sub + 1, at]),
                preferred_element_type=f32,
            )
            weight = weights_ref[sub, :, at].astype(f32)
            m_re = jnp.sum(picked[:K] * weight, 0, keepdims=True)
            m_im = jnp.sum(picked[K:] * weight, 0, keepdims=True)
            for b in range(per):
                lanes = slice(b * BLOCK, (b + 1) * BLOCK)
                samples_ref[pl.ds(2 * sub * MAXB + n * per + b, 1), :] = m_re[:, lanes]
                samples_ref[pl.ds((2 * sub + 1) * MAXB + n * per + b, 1), :] = m_im[:, lanes]
            return carry

        lax.fori_loop(0, VISITS // CHUNK, chunk, 0, unroll=2)
    out_ref[...] = samples_ref[...].astype(bf16)


def parts_of(sub):
    return (
        slice(sub * MAXB, (sub + 1) * MAXB),
        slice(2 * sub * MAXB, (2 * sub + 1) * MAXB),
        slice((2 * sub + 1) * MAXB, (2 * sub + 2) * MAXB),
    )


def observed_kernel(a_ref, b_ref, c_ref, d_ref, mix_ref, cos_ref, sin_ref, out_ref):
    for sub in range(2):
        here, re, im = parts_of(sub)
        cosine, sine = cos_ref[here, :], sin_ref[here, :]
        back_re = jnp.zeros((MAXB, BLOCK), f32)
        back_im = jnp.zeros((MAXB, BLOCK), f32)
        for corr, seen in enumerate((a_ref, b_ref, c_ref, d_ref)):
            mix = mix_ref[here, 4 * corr : 4 * corr + 1]
            back_re = back_re + mix * seen[re, :].astype(f32)
            back_im = back_im + mix * seen[im, :].astype(f32)
        out_ref[re, :] = back_re * cosine - back_im * sine
        out_ref[im, :] = back_im * cosine + back_re * sine


def mixed(mix_ref, here, first, samples):
    return sum(mix_ref[here, first + t : first + t + 1] * s for t, s in enumerate(samples))


def residual_kernel(
    counts_ref, a_ref, b_ref, c_ref, d_ref, seen_ref, mix_ref, cos_ref, sin_ref, out_ref
):
    planes = (a_ref, b_ref, c_ref, d_ref)
    block = lax.broadcasted_iota(jnp.int32, (MAXB, BLOCK), 0)
    for sub in range(2):
        live = block < counts_ref[sub]
        here, re, im = parts_of(sub)
        cosine, sine = cos_ref[here, :], sin_ref[here, :]
        m_re = mixed(mix_ref, here, 0, [p[re, :].astype(f32) for p in planes])
        m_im = mixed(mix_ref, here, 0, [p[im, :].astype(f32) for p in planes])
        left_re = jnp.where(live, seen_ref[re, :] - (m_re * cosine + m_im * sine), 0.0)
        left_im = jnp.where(live, seen_ref[im, :] - (m_im * cosine - m_re * sine), 0.0)
        for b in range(MAXB):
            lanes = slice(b * BLOCK, (b + 1) * BLOCK)
            out_ref[sub, 0:1, lanes] = left_re[b : b + 1, :]
            out_ref[sub, 1:2, lanes] = left_im[b : b + 1, :]


def adjoint_kernel(
    counts_ref, a_ref, b_ref, c_ref, d_ref, turned_ref, mix_ref, cells_ref, weights_ref,
    out_ref, back_ref,
):
    planes = (a_ref, b_ref, c_ref, d_ref)
    block = lax.broadcasted_iota(jnp.int32, (MAXB, BLOCK), 0)
    for sub in range(2):
        live = block < counts_ref[sub]
        here, re, im = parts_of(sub)
        for part in (re, im):
            samples = [p[part, :].astype(f32) for p in planes]
            back_ref[part, :] = jnp.where(
                live, turned_ref[part, :] - mixed(mix_ref, here, 16, samples), 0.0
            )
    per = CHUNK // BLOCK
    for sub in range(2):

        def chunk(n, total):
            at = pl.ds(pl.multiple_of(n * CHUNK, CHUNK), CHUNK)

            def row(part):
                base = (2 * sub + part) * MAXB + n * per
                return jnp.concatenate([back_ref[pl.ds(base + b, 1), :] for b in range(per)], 1)

            g_re, g_im = row(0), row(1)
            weight = weights_ref[sub, :, at].astype(f32)
            v_re = (g_re * weight).astype(bf16)
            v_im = (g_im * weight).astype(bf16)
            return total + nt_dot(one_hot(cells_ref[0, sub : sub + 1, at]), jnp.concatenate([v_re, v_im], 0))

        total = lax.fori_loop(0, VISITS // CHUNK, chunk, jnp.zeros((G, 2 * K), f32), unroll=2)
        out_ref[sub * 2 * K : (sub + 1) * 2 * K, :] = jnp.transpose(total).astype(bf16)


def share_kernel(
    here_ref, sub_ref, mine_ref, other_ref, lift_ref, lift_s_ref, out_ref, *tables
):
    cos_ref, sin_ref, fcos_ref, fsin_ref = tables
    sign = half_sign()
    here = here_ref[0]
    core = here & 1
    firsts = (2 * here, 2 * (here + 1 - 2 * core))
    phases([sub_ref[first + sub] for first in firsts for sub in range(2)], core, *tables)
    left = jnp.concatenate([mine_ref[...], other_ref[...]], 0)

    def pair(i, carry):
        rights = []
        for e in range(2):
            q = 2 * i + e
            rights.append(
                facet_lift(fcos_ref[pl.ds(q, 1), :], fsin_ref[pl.ds(q, 1), :], lift_ref, lift_s_ref)
            )
        product = nt_dot(left, jnp.concatenate(rights, 0))
        for e in range(2):
            q = 2 * i + e
            total = jnp.zeros((K, 2 * ROWS), f32)
            swapped = jnp.zeros((K, 2 * ROWS), f32)
            for sub in range(4):
                g_re = product[sub * 2 * K : sub * 2 * K + K, e * 128 : (e + 1) * 128]
                g_im = product[sub * 2 * K + K : (sub + 1) * 2 * K, e * 128 : (e + 1) * 128]
                pr = cos_ref[pl.ds(sub * 32 + q, 1), :]
                pi = sin_ref[pl.ds(sub * 32 + q, 1), :]
                total = total + (g_re * pr + g_im * pi)
                swapped = swapped + (g_im * pr - g_re * pi)
            out_ref[q] = (total * sign + swap(swapped)).astype(bf16)
        return carry

    lax.fori_loop(0, 16, pair, 0, unroll=4)


def image_kernel(shares_ref, column_ref, out_ref):
    total = shares_ref[0].astype(f32)
    for q in range(1, 32):
        total = total + shares_ref[q].astype(f32)
    total = total.astype(bf16).astype(f32)
    both = jnp.concatenate([total, half_sign() * swap(total)], 0)
    left = jnp.transpose(both).astype(bf16)
    image = (8.0 * jnp.dot(left, column_ref[...], preferred_element_type=f32)).astype(bf16)
    for turn in range(4):
        out_ref[:, turn * PERIOD : (turn + 1) * PERIOD] = image[:ROWS]
        out_ref[:, L + turn * PERIOD : L + (turn + 1) * PERIOD] = image[ROWS:]


def call(kernel, out_shape, scratch=(), smem=0, limit=16, flops=10**9, hbm=False):
    vmem = pl.BlockSpec(memory_space=pltpu.VMEM)

    def run(*args):
        place = pl.BlockSpec(memory_space=pltpu.HBM) if hbm else vmem
        specs = [pl.BlockSpec(memory_space=pltpu.SMEM)] * smem + [place] * (len(args) - smem)
        return pl.pallas_call(
            kernel,
            out_shape=out_shape,
            in_specs=specs,
            out_specs=jax.tree.map(lambda _: vmem, out_shape),
            scratch_shapes=list(scratch),
            cost_estimate=pl.CostEstimate(flops=flops, bytes_accessed=2**20, transcendentals=0),
            compiler_params=pltpu.CompilerParams(vmem_limit_bytes=limit * 2**20),
        )(*args)

    return run


def shape(dims, dtype):
    return jax.ShapeDtypeStruct(dims, dtype)


def column_of_subgrids(strips, sub_u, counts, uvw, mueller, observed):
    column, kernel_t, lift_t, lift_s = tables()
    column = jnp.asarray(column, bf16)
    kernel_t = jnp.asarray(kernel_t, bf16)
    lift_t = jnp.asarray(lift_t)
    lift_s = jnp.asarray(lift_s)
    here = lax.axis_index("facet")
    plane = lax.axis_index("stokes")
    groups = [[2 * q + side for q in range(32)] for side in range(2)]
    partner = [(i, i ^ 1) for i in range(FACETS)]

    def to_stokes(array):
        out = [array]
        for k in (1, 2, 3):
            out.append(lax.ppermute(array, "stokes", [(i, (i - k) % 4) for i in range(4)]))
        return out

    spread = call(
        column_kernel,
        shape((32, K, 2 * ROWS), bf16),
        (
            pltpu.VMEM((8, ROWS, PERIOD), bf16),
            pltpu.VMEM((2 * K, PERIOD), bf16),
            pltpu.SemaphoreType.DMA((9,)),
        ),
        limit=60,
        hbm=True,
    )(strips[0], column)
    mine = lax.all_to_all(spread, "facet", 0, 0, axis_index_groups=groups, tiled=True)
    square = shape((128, 128), f32)
    position = jnp.stack([here, plane])
    vcos, vsin, mix, seen, sent, weights = call(
        prepare_kernel,
        (
            square,
            square,
            square,
            shape((4 * MAXB, BLOCK), f32),
            shape((4 * MAXB, BLOCK), bf16),
            shape((2, K, VISITS), bf16),
        ),
        (pltpu.VMEM((128, 128), jnp.int32), pltpu.VMEM((128, 128), f32)),
        smem=1,
        flops=10**10,
    )(position, uvw, kernel_t, mueller, observed[0])
    turned = call(observed_kernel, shape((4 * MAXB, BLOCK), f32))(
        seen, *to_stokes(sent)[1:], mix, vcos, vsin
    )
    other = lax.ppermute(mine, "facet", partner)

    def scratch(offsets):
        return tuple(
            pltpu.VMEM(dims, f32) for dims in ((32 * offsets, 128), (32 * offsets, 128), (32, G), (32, G))
        )

    rows = call(lift_kernel, shape((4 * K, G), f32), scratch(2), smem=2)(
        position, sub_u, mine, lift_t, lift_s
    )
    samples = call(
        model_kernel,
        shape((4 * MAXB, BLOCK), bf16),
        (
            pltpu.VMEM((4 * K, G), f32),
            pltpu.VMEM((4 * K, G), bf16),
            pltpu.VMEM((4 * MAXB, BLOCK), f32),
        )
        + scratch(2),
        smem=2,
    )(position, sub_u, rows, other, lift_t, lift_s, uvw, weights)
    planes = to_stokes(samples)
    adj = call(
        adjoint_kernel,
        shape((4 * K, G), bf16),
        (pltpu.VMEM((4 * MAXB, BLOCK), f32),),
        smem=1,
    )(counts, *planes, turned, mix, uvw, weights)
    other_adj = lax.ppermute(adj, "facet", partner)
    resid = call(residual_kernel, shape((2, 2, VISITS), f32), smem=1)(
        counts, *planes, seen, mix, vcos, vsin
    )
    shares = call(share_kernel, shape((32, K, 2 * ROWS), bf16), scratch(4), smem=2)(
        position, sub_u, adj, other_adj, lift_t, lift_s
    )
    shares = lax.all_to_all(shares, "facet", 0, 0, axis_index_groups=groups, tiled=True)
    image = call(image_kernel, shape((ROWS, 2 * L), bf16))(shares, column)
    return (image[None], resid[None])


def solution(mesh):
    placed = (
        P("stokes", "facet", None),
        P(),
        P("facet"),
        P(None, "facet", None),
        P(None, None, "facet", None),
        P("stokes", "facet", None, None),
    )
    return jax.shard_map(
        column_of_subgrids,
        mesh=mesh,
        in_specs=placed,
        out_specs=(P("stokes", "facet", None), P("stokes", "facet", None, None)),
        check_vma=False,
    )
```

```python
import functools
import math

import jax
import jax.numpy as jnp
import numpy as np
from jax import lax
from jax.experimental import pallas as pl
from jax.experimental.pallas import tpu as pltpu
from jax.sharding import PartitionSpec as P


K = 64
G = 256
L = 8192
PERIOD = 2048
ROWS = 64
FACETS = 64
TOTAL = 4096
MAXB = 64
BLOCK = 128
VISITS = 8192
CHUNK = 4096
GROUP = 16

f32 = jnp.float32
bf16 = jnp.bfloat16


@functools.cache
def tables():
    lpos = np.arange(PERIOD)[None, :]
    cpos = np.arange(K)[:, None]
    angle = 2.0 * np.pi * ((4 * cpos * (lpos - 16)) % L) / L
    column = np.concatenate([np.cos(angle), -np.sin(angle)], 0) / math.sqrt(L)
    upos = np.arange(G)[:, None]
    kpos = np.arange(K)[None, :]
    mpos = np.arange(K) - K // 2
    phase = (mpos[None, None, :] * (upos - 4 * kpos)[:, :, None]) % G
    interp = np.exp(2j * np.pi * phase / G).sum(2) / (2.0 * K)
    kernel_t = (interp * np.exp(2j * np.pi * (upos - 4 * kpos) / 512)).real.T
    dpos = np.arange(ROWS) - ROWS // 2
    lift = interp @ np.exp(-2j * np.pi * np.arange(K)[:, None] * dpos[None, :] / 1024)
    lift = lift * np.exp(-2j * np.pi * upos / 128) / math.sqrt(TOTAL)
    lift_t = np.concatenate([lift.real.T, lift.imag.T], 0)
    lift_s = np.concatenate([-lift.imag.T, lift.real.T], 0)
    return (
        column.astype(np.float32),
        kernel_t.astype(np.float32),
        lift_t.astype(np.float32),
        lift_s.astype(np.float32),
    )


def half_sign():
    lane = lax.broadcasted_iota(jnp.int32, (1, 2 * K), 1)
    return jnp.where(lane < K, 1.0, -1.0).astype(f32)


def swap(x):
    return pltpu.roll(x, K, 1)


def one_hot(cells):
    grid_pos = lax.broadcasted_iota(jnp.int32, (G, cells.shape[1]), 0)
    return jnp.where(grid_pos == cells, 1.0, 0.0).astype(bf16)


def nt_dot(a, b):
    return lax.dot_general(a, b, (((1,), (1,)), ((), ())), preferred_element_type=f32)


def column_kernel(strips_ref, column_ref, out_ref, strips_buf, column_buf, sems):
    copies = [
        pltpu.make_async_copy(
            strips_ref.at[:, pl.ds(i * PERIOD, PERIOD)], strips_buf.at[i], sems.at[i]
        )
        for i in range(8)
    ]
    table = pltpu.make_async_copy(column_ref, column_buf, sems.at[8])
    for copy in copies:
        copy.start()
    table.start()
    parts = []
    for part in range(2):
        copies[4 * part].wait()
        copies[4 * part + 1].wait()
        folded = strips_buf[4 * part].astype(f32) + strips_buf[4 * part + 1].astype(f32)
        copies[4 * part + 2].wait()
        copies[4 * part + 3].wait()
        folded = folded + strips_buf[4 * part + 2].astype(f32) + strips_buf[4 * part + 3].astype(f32)
        parts.append(folded.astype(bf16))
    table.wait()
    product = nt_dot(column_buf[...], jnp.concatenate(parts, 0))
    coeffs = (product[:K] - half_sign() * swap(product[K:])).astype(bf16)
    for q in range(32):
        out_ref[q] = coeffs


def turn(n, period):
    t = n.astype(f32) * (4.0 / period)
    q = jnp.floor(t + 0.5)
    x = (t - q) * (math.pi / 2)
    quarter = q.astype(jnp.int32) & 3
    y = x * x
    s = x * (1.0 + y * (-1.0 / 6 + y * (1.0 / 120 + y * (-1.0 / 5040 + y * (1.0 / 362880)))))
    c = 1.0 + y * (-0.5 + y * (1.0 / 24 + y * (-1.0 / 720 + y * (1.0 / 40320))))
    odd = (quarter & 1) == 1
    cosine = jnp.where(odd, s, c)
    sine = jnp.where(odd, c, s)
    cosine = jnp.where((quarter == 1) | (quarter == 2), -cosine, cosine)
    sine = jnp.where(quarter >= 2, sine, -sine)
    return cosine, sine


def prepare_kernel(
    here_ref, cells_ref, kernel_ref, mueller_ref, observed_ref, vcos_ref, vsin_ref, mix_ref, seen_ref,
    sent_ref, weights_ref, steps_ref, rows_ref,
):
    plane = here_ref[1]
    for sub in range(2):
        for b in range(MAXB):
            lanes = slice(b * BLOCK, (b + 1) * BLOCK)
            steps_ref[sub * MAXB + b : sub * MAXB + b + 1, :] = (
                2 * cells_ref[2, sub : sub + 1, lanes] + cells_ref[1, sub : sub + 1, lanes]
            )
            for part in range(2):
                at = (2 * sub + part) * MAXB + b
                seen_ref[at : at + 1, :] = observed_ref[sub, part : part + 1, lanes]
    sent_ref[...] = seen_ref[...].astype(bf16)
    cosine, sine = turn(steps_ref[...] & (2 * G - 1), 2 * G)
    vcos_ref[...] = cosine
    vsin_ref[...] = -sine
    rows_ref[...] = jnp.zeros_like(rows_ref)
    for corr in range(4):
        for t in range(4):
            entry = mueller_ref[(plane + corr) & 3, (plane + t) & 3]
            at = 4 * corr + t
            rows_ref[at : at + 1, :] = jnp.concatenate([entry[0:1, :], entry[1:2, :]], 1)
    for t in range(4):
        rows_ref[16 + t : 17 + t, :] = sum(
            rows_ref[4 * corr : 4 * corr + 1, :] * rows_ref[4 * corr + t : 4 * corr + t + 1, :]
            for corr in range(4)
        )
    mix_ref[...] = jnp.transpose(rows_ref[...])
    for sub in range(2):

        def chunk(n, carry):
            at = pl.ds(pl.multiple_of(n * CHUNK, CHUNK), CHUNK)
            picked = jnp.dot(
                kernel_ref[...], one_hot(cells_ref[1, sub : sub + 1, at]), preferred_element_type=f32
            )
            weights_ref[sub, :, at] = picked.astype(bf16)
            return carry

        lax.fori_loop(0, VISITS // CHUNK, chunk, 0, unroll=2)


def phases(offsets, parity, cos_ref, sin_ref, fcos_ref, fsin_ref):
    step = lax.broadcasted_iota(jnp.int32, (32, 2 * ROWS), 0)
    lane = lax.broadcasted_iota(jnp.int32, (32, 2 * ROWS), 1) & (ROWS - 1)
    rows = (2 * step + parity) * ROWS + lane
    for i, offset in enumerate(offsets):
        cosine, sine = turn((rows * offset) & (TOTAL - 1), TOTAL)
        cos_ref[32 * i : 32 * i + 32, :] = cosine
        sin_ref[32 * i : 32 * i + 32, :] = sine
    step = lax.broadcasted_iota(jnp.int32, (32, G), 0)
    lane = lax.broadcasted_iota(jnp.int32, (32, G), 1)
    cosine, sine = turn(((2 * step + parity) * lane) & (FACETS - 1), FACETS)
    fcos_ref[...] = cosine
    fsin_ref[...] = sine


def facet_lift(cos_row, sin_row, lift_ref, lift_s_ref):
    return (cos_row * lift_ref[...] + sin_row * lift_s_ref[...]).astype(bf16)


def lift(here_ref, sub_ref, side, source, lift_ref, lift_s_ref, total_ref, tables):
    cos_ref, sin_ref, fcos_ref, fsin_ref = tables
    here = here_ref[0]
    core = here & 1
    offsets = [sub_ref[2 * here + sub] for sub in range(2)]
    phases(offsets, core if side == 0 else 1 - core, *tables)
    sign = half_sign()

    def group(i, carry):
        lefts, rights = [], []
        for e in range(GROUP):
            q = GROUP * i + e
            first = source[q].astype(f32)
            second = swap(first)
            rights.append(
                facet_lift(fcos_ref[pl.ds(q, 1), :], fsin_ref[pl.ds(q, 1), :], lift_ref, lift_s_ref)
            )
            blocks = []
            for sub in range(2):
                pr = cos_ref[pl.ds(sub * 32 + q, 1), :]
                pi = sin_ref[pl.ds(sub * 32 + q, 1), :]
                blocks.append((first * (pr * sign) - second * pi).astype(bf16))
                blocks.append((second * pr + first * (pi * sign)).astype(bf16))
            lefts.append(jnp.concatenate(blocks, 0))
        left = jnp.concatenate(lefts, 1)
        right = jnp.concatenate(rights, 0)
        total_ref[...] += jnp.dot(left, right, preferred_element_type=f32)
        return carry

    lax.fori_loop(0, 32 // GROUP, group, 0)


def lift_kernel(here_ref, sub_ref, mine_ref, lift_ref, lift_s_ref, rows_ref, *tables):
    rows_ref[...] = jnp.zeros_like(rows_ref)
    lift(here_ref, sub_ref, 0, mine_ref, lift_ref, lift_s_ref, rows_ref, tables)


def model_kernel(
    here_ref, sub_ref, start_ref, other_ref, lift_ref, lift_s_ref, cells_ref, weights_ref,
    out_ref, rows_ref, lifted_ref, samples_ref, *tables
):
    rows_ref[...] = start_ref[...]
    lift(here_ref, sub_ref, 1, other_ref, lift_ref, lift_s_ref, rows_ref, tables)
    lifted_ref[...] = rows_ref[...].astype(bf16)
    per = CHUNK // BLOCK
    for sub in range(2):

        def chunk(n, carry):
            at = pl.ds(pl.multiple_of(n * CHUNK, CHUNK), CHUNK)
            picked = jnp.dot(
                lifted_ref[sub * 2 * K : (sub + 1) * 2 * K, :],
                one_hot(cells_ref[0, sub : sub + 1, at]),
                preferred_element_type=f32,
            )
            weight = weights_ref[sub, :, at].astype(f32)
            m_re = jnp.sum(picked[:K] * weight, 0, keepdims=True)
            m_im = jnp.sum(picked[K:] * weight, 0, keepdims=True)
            for b in range(per):
                lanes = slice(b * BLOCK, (b + 1) * BLOCK)
                samples_ref[pl.ds(2 * sub * MAXB + n * per + b, 1), :] = m_re[:, lanes]
                samples_ref[pl.ds((2 * sub + 1) * MAXB + n * per + b, 1), :] = m_im[:, lanes]
            return carry

        lax.fori_loop(0, VISITS // CHUNK, chunk, 0, unroll=2)
    out_ref[...] = samples_ref[...].astype(bf16)


def parts_of(sub):
    return (
        slice(sub * MAXB, (sub + 1) * MAXB),
        slice(2 * sub * MAXB, (2 * sub + 1) * MAXB),
        slice((2 * sub + 1) * MAXB, (2 * sub + 2) * MAXB),
    )


def observed_kernel(a_ref, b_ref, d_ref, c_ref, mix_ref, cos_ref, sin_ref, out_ref):
    for sub in range(2):
        here, re, im = parts_of(sub)
        cosine, sine = cos_ref[here, :], sin_ref[here, :]
        back_re = jnp.zeros((MAXB, BLOCK), f32)
        back_im = jnp.zeros((MAXB, BLOCK), f32)
        for corr, seen in enumerate((a_ref, b_ref, c_ref, d_ref)):
            mix = mix_ref[here, 4 * corr : 4 * corr + 1]
            back_re = back_re + mix * seen[re, :].astype(f32)
            back_im = back_im + mix * seen[im, :].astype(f32)
        out_ref[re, :] = back_re * cosine - back_im * sine
        out_ref[im, :] = back_im * cosine + back_re * sine


def mixed(mix_ref, here, first, samples):
    return sum(mix_ref[here, first + t : first + t + 1] * s for t, s in enumerate(samples))


def residual_kernel(
    counts_ref, a_ref, b_ref, d_ref, c_ref, seen_ref, mix_ref, cos_ref, sin_ref, out_ref
):
    planes = (a_ref, b_ref, c_ref, d_ref)
    block = lax.broadcasted_iota(jnp.int32, (MAXB, BLOCK), 0)
    for sub in range(2):
        live = block < counts_ref[sub]
        here, re, im = parts_of(sub)
        cosine, sine = cos_ref[here, :], sin_ref[here, :]
        m_re = mixed(mix_ref, here, 0, [p[re, :].astype(f32) for p in planes])
        m_im = mixed(mix_ref, here, 0, [p[im, :].astype(f32) for p in planes])
        left_re = jnp.where(live, seen_ref[re, :] - (m_re * cosine + m_im * sine), 0.0)
        left_im = jnp.where(live, seen_ref[im, :] - (m_im * cosine - m_re * sine), 0.0)
        for b in range(MAXB):
            lanes = slice(b * BLOCK, (b + 1) * BLOCK)
            out_ref[sub, 0:1, lanes] = left_re[b : b + 1, :]
            out_ref[sub, 1:2, lanes] = left_im[b : b + 1, :]


def adjoint_kernel(
    counts_ref, a_ref, b_ref, d_ref, c_ref, turned_ref, mix_ref, cells_ref, weights_ref,
    out_ref, back_ref,
):
    planes = (a_ref, b_ref, c_ref, d_ref)
    block = lax.broadcasted_iota(jnp.int32, (MAXB, BLOCK), 0)
    for sub in range(2):
        live = block < counts_ref[sub]
        here, re, im = parts_of(sub)
        for part in (re, im):
            samples = [p[part, :].astype(f32) for p in planes]
            back_ref[part, :] = jnp.where(
                live, turned_ref[part, :] - mixed(mix_ref, here, 16, samples), 0.0
            )
    per = CHUNK // BLOCK
    for sub in range(2):

        def chunk(n, total):
            at = pl.ds(pl.multiple_of(n * CHUNK, CHUNK), CHUNK)

            def row(part):
                base = (2 * sub + part) * MAXB + n * per
                return jnp.concatenate([back_ref[pl.ds(base + b, 1), :] for b in range(per)], 1)

            g_re, g_im = row(0), row(1)
            weight = weights_ref[sub, :, at].astype(f32)
            v_re = (g_re * weight).astype(bf16)
            v_im = (g_im * weight).astype(bf16)
            return total + nt_dot(one_hot(cells_ref[0, sub : sub + 1, at]), jnp.concatenate([v_re, v_im], 0))

        total = lax.fori_loop(0, VISITS // CHUNK, chunk, jnp.zeros((G, 2 * K), f32), unroll=2)
        out_ref[sub * 2 * K : (sub + 1) * 2 * K, :] = jnp.transpose(total).astype(bf16)


def share_kernel(
    here_ref, sub_ref, mine_ref, other_ref, lift_ref, lift_s_ref, out_ref, *tables
):
    cos_ref, sin_ref, fcos_ref, fsin_ref = tables
    sign = half_sign()
    here = here_ref[0]
    core = here & 1
    firsts = (2 * here, 2 * (here + 1 - 2 * core))
    phases([sub_ref[first + sub] for first in firsts for sub in range(2)], core, *tables)
    left = jnp.concatenate([mine_ref[...], other_ref[...]], 0)

    def pair(i, carry):
        rights = []
        for e in range(2):
            q = 2 * i + e
            rights.append(
                facet_lift(fcos_ref[pl.ds(q, 1), :], fsin_ref[pl.ds(q, 1), :], lift_ref, lift_s_ref)
            )
        product = nt_dot(left, jnp.concatenate(rights, 0))
        for e in range(2):
            q = 2 * i + e
            total = jnp.zeros((K, 2 * ROWS), f32)
            swapped = jnp.zeros((K, 2 * ROWS), f32)
            for sub in range(4):
                g_re = product[sub * 2 * K : sub * 2 * K + K, e * 128 : (e + 1) * 128]
                g_im = product[sub * 2 * K + K : (sub + 1) * 2 * K, e * 128 : (e + 1) * 128]
                pr = cos_ref[pl.ds(sub * 32 + q, 1), :]
                pi = sin_ref[pl.ds(sub * 32 + q, 1), :]
                total = total + (g_re * pr + g_im * pi)
                swapped = swapped + (g_im * pr - g_re * pi)
            out_ref[q] = (total * sign + swap(swapped)).astype(bf16)
        return carry

    lax.fori_loop(0, 16, pair, 0, unroll=8)


def image_kernel(shares_ref, column_ref, out_ref):
    total = shares_ref[0].astype(f32)
    for q in range(1, 32):
        total = total + shares_ref[q].astype(f32)
    total = total.astype(bf16).astype(f32)
    both = jnp.concatenate([total, half_sign() * swap(total)], 0)
    left = jnp.transpose(both).astype(bf16)
    image = (8.0 * jnp.dot(left, column_ref[...], preferred_element_type=f32)).astype(bf16)
    for turn in range(4):
        out_ref[:, turn * PERIOD : (turn + 1) * PERIOD] = image[:ROWS]
        out_ref[:, L + turn * PERIOD : L + (turn + 1) * PERIOD] = image[ROWS:]


def call(kernel, out_shape, scratch=(), smem=0, limit=16, flops=10**9, hbm=False):
    vmem = pl.BlockSpec(memory_space=pltpu.VMEM)

    def run(*args):
        place = pl.BlockSpec(memory_space=pltpu.HBM) if hbm else vmem
        specs = [pl.BlockSpec(memory_space=pltpu.SMEM)] * smem + [place] * (len(args) - smem)
        return pl.pallas_call(
            kernel,
            out_shape=out_shape,
            in_specs=specs,
            out_specs=jax.tree.map(lambda _: vmem, out_shape),
            scratch_shapes=list(scratch),
            cost_estimate=pl.CostEstimate(flops=flops, bytes_accessed=2**20, transcendentals=0),
            compiler_params=pltpu.CompilerParams(vmem_limit_bytes=limit * 2**20),
        )(*args)

    return run


def shape(dims, dtype):
    return jax.ShapeDtypeStruct(dims, dtype)


def column_of_subgrids(strips, sub_u, counts, uvw, mueller, observed):
    column, kernel_t, lift_t, lift_s = tables()
    column = jnp.asarray(column, bf16)
    kernel_t = jnp.asarray(kernel_t, bf16)
    lift_t = jnp.asarray(lift_t)
    lift_s = jnp.asarray(lift_s)
    here = lax.axis_index("facet")
    plane = lax.axis_index("stokes")
    groups = [[2 * q + side for q in range(32)] for side in range(2)]
    partner = [(i, i ^ 1) for i in range(FACETS)]

    def to_stokes(array):
        out = [array] * 4
        for k in (1, 2, 3):
            out[k] = lax.ppermute(array, "stokes", [(i, (i - k) % 4) for i in range(4)])
        return [out[0], out[1], out[3], out[2]]

    spread = call(
        column_kernel,
        shape((32, K, 2 * ROWS), bf16),
        (
            pltpu.VMEM((8, ROWS, PERIOD), bf16),
            pltpu.VMEM((2 * K, PERIOD), bf16),
            pltpu.SemaphoreType.DMA((9,)),
        ),
        limit=60,
        hbm=True,
    )(strips[0], column)
    mine = lax.all_to_all(spread, "facet", 0, 0, axis_index_groups=groups, tiled=True)
    square = shape((128, 128), f32)
    position = jnp.stack([here, plane])
    vcos, vsin, mix, seen, sent, weights = call(
        prepare_kernel,
        (
            square,
            square,
            square,
            shape((4 * MAXB, BLOCK), f32),
            shape((4 * MAXB, BLOCK), bf16),
            shape((2, K, VISITS), bf16),
        ),
        (pltpu.VMEM((128, 128), jnp.int32), pltpu.VMEM((128, 128), f32)),
        smem=1,
        flops=10**10,
    )(position, uvw, kernel_t, mueller, observed[0])
    turned = call(observed_kernel, shape((4 * MAXB, BLOCK), f32))(
        seen, *to_stokes(sent)[1:], mix, vcos, vsin
    )
    other = lax.ppermute(mine, "facet", partner)

    def scratch(offsets):
        return tuple(
            pltpu.VMEM(dims, f32) for dims in ((32 * offsets, 128), (32 * offsets, 128), (32, G), (32, G))
        )

    rows = call(lift_kernel, shape((4 * K, G), f32), scratch(2), smem=2)(
        position, sub_u, mine, lift_t, lift_s
    )
    samples = call(
        model_kernel,
        shape((4 * MAXB, BLOCK), bf16),
        (
            pltpu.VMEM((4 * K, G), f32),
            pltpu.VMEM((4 * K, G), bf16),
            pltpu.VMEM((4 * MAXB, BLOCK), f32),
        )
        + scratch(2),
        smem=2,
    )(position, sub_u, rows, other, lift_t, lift_s, uvw, weights)
    planes = to_stokes(samples)
    adj = call(
        adjoint_kernel,
        shape((4 * K, G), bf16),
        (pltpu.VMEM((4 * MAXB, BLOCK), f32),),
        smem=1,
    )(counts, *planes, turned, mix, uvw, weights)
    other_adj = lax.ppermute(adj, "facet", partner)
    resid = call(residual_kernel, shape((2, 2, VISITS), f32), smem=1)(
        counts, *planes, seen, mix, vcos, vsin
    )
    shares = call(share_kernel, shape((32, K, 2 * ROWS), bf16), scratch(4), smem=2)(
        position, sub_u, adj, other_adj, lift_t, lift_s
    )
    shares = lax.all_to_all(shares, "facet", 0, 0, axis_index_groups=groups, tiled=True)
    image = call(image_kernel, shape((ROWS, 2 * L), bf16))(shares, column)
    return (image[None], resid[None])


def solution(mesh):
    placed = (
        P("stokes", "facet", None),
        P(),
        P("facet"),
        P(None, "facet", None),
        P(None, None, "facet", None),
        P("stokes", "facet", None, None),
    )
    return jax.shard_map(
        column_of_subgrids,
        mesh=mesh,
        in_specs=placed,
        out_specs=(P("stokes", "facet", None), P("stokes", "facet", None, None)),
        check_vma=False,
    )
```
